256 devices in a mesh: grp: 2 (over z_hi), gy: 4 (over z_lo), gz: 32 (over x, y, core).
Axes of the slice: x: 4, y: 4, z: 8 (z_hi: 2, z_lo: 4; z = z_hi * 4 + z_lo), core: 2. Of those that a mesh axis runs over, the one named last changes fastest.
Arguments:
- vorticity: float32 [2, 3, 256, 256, 256], P('grp', None, 'gz', 'gy'), may hold values from -6 to 6
- wind: float32 [2, 3], P('grp'), may hold values from 0.5 to 1.2
Outputs:
- new_vorticity: float32 [2, 3, 256, 256, 256], P('grp', None, 'gz', 'gy')
- velocity: float32 [2, 3, 256, 256, 256], P('grp', None, 'gz', 'gy')
The draws below stay inside these ranges and needn't reach their ends.
All inputs are finite; a program needn't handle non-finite values.
Results may differ from the reference program's by a relative error of at most 0.0003.
Values sent between devices are 32-bit elements; how exact they have to be, the bound alone decides.
A program may use at most 128 MiB of HBM per device.

```python
import math
import jax
import jax.numpy as jnp

NX = 256
NY = 256
NZ = 256


def draw_vorticity(key, part):
    shape = (2, 3, NZ, NY, NX)
    first = jax.random.fold_in(key, 0)
    return jnp.clip(jax.random.normal(first, shape, jnp.float32), -6.0, 6.0)


def shard_levels(key, shape, cuts, smallest, largest):
    def one(position, parts):
        steps = jax.random.uniform(jax.random.fold_in(jax.random.fold_in(key, 6), position), (parts,), jnp.float32, smallest / len(cuts), largest / len(cuts))
        return jnp.repeat(jnp.exp(steps), shape[position] // parts).reshape((-1,) + (1,) * (len(shape) - position - 1))

    gain = one(*cuts[0])
    for cut in cuts[1:]:
        gain = gain * one(*cut)
    return gain


def setup_inputs(seed: int = 0) -> dict:
    key_of = jax.random.split(jax.random.key(seed), 3)
    vorticity = draw_vorticity(jax.random.fold_in(key_of[2], 71), 0)
    wind = jnp.clip(0.5 + 0.70000005 * jax.random.uniform(key_of[1], (2, 3), jnp.float32) ** shard_levels(key_of[1], (2, 3), ((0, 2),), -0.2, 0.2), 0.5, 1.2)
    return dict(vorticity=vorticity, wind=wind)


TIME_STEP = 0.4


def kernel_weight(offset):
    mag = jnp.abs(offset)
    inner = 1.0 - 2.5 * mag * mag + 1.5 * mag * mag * mag
    outer = 0.5 * (2.0 - mag) * (2.0 - mag) * (1.0 - mag)
    return jnp.where(mag < 1.0, inner, jnp.where(mag < 2.0, outer, 0.0 * mag))


def wave_numbers(count):
    index = jnp.arange(count, dtype=jnp.int32)
    signed = jnp.where(index < count // 2, index, index - count)
    return signed.astype(jnp.float32) * (2.0 * math.pi / count)


def velocity_of(field, drift):
    spectrum = jnp.fft.fftn(field, axes=(1, 2, 3))
    wave_z = wave_numbers(NZ)[:, None, None]
    wave_y = wave_numbers(NY)[None, :, None]
    wave_x = wave_numbers(NX)[None, None, :]
    squared = wave_x * wave_x + wave_y * wave_y + wave_z * wave_z
    inverse = jnp.where(squared > 0, 1.0 / jnp.where(squared > 0, squared, 1.0), 0.0 * squared)
    stream = spectrum * inverse
    cross_x = wave_y * stream[2] - wave_z * stream[1]
    cross_y = wave_z * stream[0] - wave_x * stream[2]
    cross_z = wave_x * stream[1] - wave_y * stream[0]
    result = jnp.real(jnp.fft.ifftn(1j * jnp.stack([cross_x, cross_y, cross_z]), axes=(1, 2, 3)))
    return result + drift[:, None, None, None]


def central(values, axis):
    return (jnp.roll(values, -1, axis) - jnp.roll(values, 1, axis)) * 0.5


def stretch(field, speed, grad_x):
    grad_y = central(speed, 2)
    grad_z = central(speed, 1)
    return field + TIME_STEP * (field[0:1] * grad_x + field[1:2] * grad_y + field[2:3] * grad_z)


def remesh_periodic(values, shift, axis):
    total = jnp.zeros_like(values)
    for offset in range(-2, 3):
        total = total + jnp.roll(values, offset, axis) * kernel_weight(offset - jnp.roll(shift, offset, axis))
    return total


def remesh_inflow(values, shift, ghost_values, ghost_shift):
    q_ext = jnp.concatenate([ghost_values, values, jnp.zeros_like(values[..., :2])], -1)
    d_ext = jnp.concatenate([ghost_shift, shift, jnp.zeros_like(shift[..., :2])], -1)
    total = jnp.zeros_like(values)
    for offset in range(-2, 3):
        start = 2 - offset
        total = total + q_ext[..., start:start + NX] * kernel_weight(offset - d_ext[..., start:start + NX])
    return total


def reference(vorticity, wind):
    speed_pre = velocity_of(vorticity[0], wind[0])
    speed_wake = velocity_of(vorticity[1], wind[1])
    strength_pre = stretch(vorticity[0], speed_pre, central(speed_pre, 3))
    extended = jnp.concatenate([speed_pre[..., NX - 1:], speed_wake, speed_wake[..., NX - 1:]], -1)
    grad_wake = (extended[..., 2:] - extended[..., :-2]) * 0.5
    strength_wake = stretch(vorticity[1], speed_wake, grad_wake)
    moved_pre = remesh_periodic(strength_pre, TIME_STEP * speed_pre[0:1], 3)
    moved_wake = remesh_inflow(strength_wake, TIME_STEP * speed_wake[0:1], strength_pre[..., NX - 2:], TIME_STEP * speed_pre[0:1][..., NX - 2:])
    outputs = []
    for moved, speed in ((moved_pre, speed_pre), (moved_wake, speed_wake)):
        lateral = remesh_periodic(moved, TIME_STEP * speed[1:2], 2)
        outputs.append(remesh_periodic(lateral, TIME_STEP * speed[2:3], 1))
    return jnp.stack(outputs), jnp.stack([speed_pre, speed_wake])
```

```python
import functools
import math

import jax
import jax.numpy as jnp
import numpy as np
from jax import lax
from jax.experimental import pallas as pl
from jax.experimental.pallas import tpu as pltpu
from jax.sharding import PartitionSpec as P

TIME_STEP = 0.4
MESH = pl.DeviceIdType.MESH
N = 256
HALF = 128
GY = 4
GZ = 32
PEERS = GY * GZ
LZ = 8
LY = 64


def split(values):
    high = values.astype(jnp.bfloat16)
    low = (values - high.astype(jnp.float32)).astype(jnp.bfloat16)
    return high, low


def table_pair(table):
    table = np.asarray(table, np.float32)
    high = table.astype(jnp.bfloat16)
    low = (table - high.astype(np.float32)).astype(jnp.bfloat16)
    return np.stack([high, low])


def make_tables():
    index = np.arange(N)
    angle = (index[:, None] * index[None, :] % N) * (2.0 * math.pi / N)
    cosine, sine = np.cos(angle), np.sin(angle)
    alternate = 1.0 - 2.0 * (index % 2)
    sine_in = -sine[:HALF].copy()
    sine_in[0] = alternate
    x_in = np.concatenate([cosine[:HALF], sine_in], 0)
    x_out = 2.0 * x_in / N
    x_out[0] *= 0.5
    x_out[HALF] *= 0.5
    cos_y = cosine.reshape(GY, 1, LY, N)
    sin_y = sine.reshape(GY, 1, LY, N)
    to_real = np.concatenate([cos_y, sin_y], 1).reshape(2 * N, N)
    to_imag = np.concatenate([-sin_y, cos_y], 1).reshape(2 * N, N)
    y_in = np.concatenate([to_real, to_imag], 1)
    y_out = np.concatenate([to_real, to_imag], 1).T / N
    z_all = np.stack([cosine, sine])
    return [table_pair(t) for t in (x_in, y_in, z_all, y_out, x_out)]


def dot3(a, b, dims=((1,), (0,))):
    def one(left, right):
        return lax.dot_general(left, right, (dims, ((), ())), preferred_element_type=jnp.float32)

    return one(a[0], b[0]) + (one(a[0], b[1]) + one(a[1], b[0]))


def each_peer(gy, gz, visit):
    for q in range(1, GY):
        visit(lax.rem(gy + q, GY), gz)

    def step(k, carry):
        other_z = lax.rem(gz + k, GZ)
        for q in range(GY):
            visit(lax.rem(gy + q, GY), other_z)
        return carry

    lax.fori_loop(1, GZ, step, 0)


def wait_bytes(ref, sem):
    pltpu.make_async_copy(ref, ref, sem).wait()


def waves(shape, axis):
    index = lax.broadcasted_iota(jnp.int32, shape, axis)
    signed = jnp.where(index < N // 2, index, index - N)
    full = signed.astype(jnp.float32) * (2.0 * math.pi / N)
    return full, jnp.where(index == N // 2, 0.0, full)


def spectral_kernel(
    field, wind, x_in, y_in, z_all, y_out, x_out, velocity,
    send, recv, stream, send2, recv2, scale, ssem, rsem, ssem2, rsem2,
):
    gy = lax.axis_index("gy")
    gz = lax.axis_index("gz")
    me = gy * GZ + gz
    barrier = pltpu.get_barrier_semaphore()

    def greet(other_y, other_z):
        pl.semaphore_signal(
            barrier, inc=1, device_id={"gy": other_y, "gz": other_z}, device_id_type=MESH
        )

    each_peer(gy, gz, greet)

    lane = lax.broadcasted_iota(jnp.int32, (HALF, 128), 1)
    first_half = lane < LY
    for c in (1, 2, 0):
        for b in range(2):
            rows = field[0, c, 4 * b : 4 * b + 4].reshape(4 * LY, N)
            lines = dot3((x_in[0], x_in[1]), split(rows), ((1,), (1,)))
            for t in range(2):
                real = lines[:HALF, 128 * t : 128 * t + 128]
                imag = lines[HALF:, 128 * t : 128 * t + 128]
                even = jnp.where(first_half, real, pltpu.roll(imag, LY, 1))
                odd = jnp.where(first_half, pltpu.roll(real, LY, 1), imag)
                z = 4 * b + 2 * t
                send[c, pl.ds(z, HALF, stride=LZ), :] = even
                send[c, pl.ds(z + 1, HALF, stride=LZ), :] = odd
    mine = pl.ds(pl.multiple_of(me * LZ, LZ), LZ)
    mine_z = pl.ds(pl.multiple_of(gz * LZ, LZ), LZ)
    pl.semaphore_wait(barrier, PEERS - 1)

    for c in (1, 2, 0):
        def out(other_y, other_z, c=c):
            other = other_y * GZ + other_z
            pltpu.make_async_remote_copy(
                send.at[c, pl.ds(pl.multiple_of(other * LZ, LZ), LZ)],
                recv.at[c, gy, mine_z],
                ssem.at[c],
                rsem.at[c],
                device_id={"gy": other_y, "gz": other_z},
                device_id_type=MESH,
            ).start()

        each_peer(gy, gz, out)
        recv[c, gy, mine_z, :] = send[c, mine, :]

    wave_z, curl_z = waves((N, N), 0)
    wave_y, curl_y = waves((N, N), 1)
    curl_x = me.astype(jnp.float32) * (2.0 * math.pi / N)
    squared = curl_x * curl_x + wave_y * wave_y + wave_z * wave_z
    positive = squared > 0
    scale[0] = jnp.where(positive, 1.0 / jnp.where(positive, squared, 1.0), 0.0)

    @pl.when(me == 0)
    def _():
        base = scale[0]
        top = 1.0 / (squared + math.pi * math.pi)
        scale[0] = 0.5 * (base + top)
        scale[1] = 0.5 * (base - top)

    curl = (curl_x, curl_y, curl_z)
    table_y = (y_in[0], y_in[1])
    cosine = (z_all[0, 0], z_all[1, 0])
    sine = (z_all[0, 1], z_all[1, 1])

    def transform(plane):
        lines = split(dot3(split(plane), table_y))
        by_cos = dot3(cosine, lines)
        by_sin = dot3(sine, lines)
        real = by_cos[:, :N] + by_sin[:, N:]
        imag = by_cos[:, N:] - by_sin[:, :N]
        return real, imag

    def forward(c):
        wait_bytes(recv2.at[c, pl.ds(0, (PEERS - 1) * LZ)], rsem.at[c])
        plane = jnp.concatenate([recv[c, j] for j in range(GY)], 1)
        real, imag = transform(plane)
        stream[c, 0] = real * scale[0]
        stream[c, 1] = imag * scale[0]

        @pl.when(me == 0)
        def _():
            column = lax.broadcasted_iota(jnp.int32, (N, 2 * N), 1)
            plane = jnp.concatenate([recv[c, j] for j in range(GY)], 1)
            real, imag = transform(jnp.where(column % 128 < LY, plane, -plane))
            stream[c, 0] += real * scale[1]
            stream[c, 1] += imag * scale[1]

    def backward(d):
        a, b = (d + 1) % 3, (d + 2) % 3
        real = curl[b] * stream[a, 1] - curl[a] * stream[b, 1]
        imag = curl[a] * stream[b, 0] - curl[b] * stream[a, 0]
        lines = split(jnp.concatenate([real, imag], 1))
        by_cos = dot3(cosine, lines)
        by_sin = dot3(sine, lines)
        real = by_cos[:, :N] - by_sin[:, N:]
        imag = by_cos[:, N:] + by_sin[:, :N]
        lines = split(jnp.concatenate([real, imag], 1) * (1.0 / N))
        plane = dot3(lines, (y_out[0], y_out[1]))
        for j in range(GY):
            send2[d, j] = plane[:, 128 * j : 128 * j + 128]

        def out(other_y, other_z):
            pltpu.make_async_remote_copy(
                send2.at[d, other_y, pl.ds(pl.multiple_of(other_z * LZ, LZ), LZ)],
                recv2.at[d, mine],
                ssem2.at[d],
                rsem2.at[d],
                device_id={"gy": other_y, "gz": other_z},
                device_id_type=MESH,
            ).start()

        each_peer(gy, gz, out)
        recv2[d, mine, :] = send2[d, gy, mine_z, :]

    forward(1)
    forward(2)
    backward(0)
    forward(0)
    backward(1)
    backward(2)

    for d in range(3):
        wait_bytes(recv2.at[d, pl.ds(0, (PEERS - 1) * LZ)], rsem2.at[d])
        drift = wind[0, d]
        for b in range(2):
            parts = []
            for z in range(4 * b, 4 * b + 4):
                turned = recv2[d, pl.ds(z, HALF, stride=LZ), :].T
                parts.append(jnp.concatenate([turned[:LY], turned[LY:]], 1))
            lines = split(jnp.concatenate(parts, 0))
            out = dot3(lines, (x_out[0], x_out[1])) + drift
            velocity[0, d, 4 * b : 4 * b + 4] = out.reshape(4, LY, N)

    for c in range(3):
        wait_bytes(send.at[c, pl.ds(0, (PEERS - 1) * LZ)], ssem.at[c])
        wait_bytes(send.at[c, pl.ds(0, (PEERS - 1) * LZ)], ssem2.at[c])


def spectral_velocity(vorticity, wind):
    tables = [jnp.asarray(t) for t in make_tables()]
    vmem = pl.BlockSpec(memory_space=pltpu.VMEM)
    return pl.pallas_call(
        spectral_kernel,
        out_shape=jax.ShapeDtypeStruct(vorticity.shape, jnp.float32),
        in_specs=[vmem, pl.BlockSpec(memory_space=pltpu.SMEM)] + [vmem] * 5,
        out_specs=vmem,
        scratch_shapes=[
            pltpu.VMEM((3, PEERS * LZ, 128), jnp.float32),
            pltpu.VMEM((3, GY, N, 128), jnp.float32),
            pltpu.VMEM((3, 2, N, N), jnp.float32),
            pltpu.VMEM((3, GY, N, 128), jnp.float32),
            pltpu.VMEM((3, PEERS * LZ, 128), jnp.float32),
            pltpu.VMEM((2, N, N), jnp.float32),
            pltpu.SemaphoreType.DMA((3,)),
            pltpu.SemaphoreType.DMA((3,)),
            pltpu.SemaphoreType.DMA((3,)),
            pltpu.SemaphoreType.DMA((3,)),
        ],
        compiler_params=pltpu.CompilerParams(collective_id=0, has_side_effects=True),
    )(vorticity, wind, *tables)


def shifted(value, axis, steps):
    count = lax.axis_size(axis)
    initial, last = (max(0, -steps), min(count, count - steps))
    return lax.ppermute(value, axis, [(source, source + steps) for source in range(initial, last)])


def padded(array, sides, width):
    edges = {}
    for axis, dim in sides:
        devices, length = (lax.axis_size(axis), array.shape[dim])
        up = [(i, (i + 1) % devices) for i in range(devices)]
        last = lax.slice_in_dim(array, length - width, length, axis=dim)
        initial = lax.slice_in_dim(array, 0, width, axis=dim)
        edges[dim] = (
            lax.ppermute(last, axis, up),
            lax.ppermute(initial, axis, [(b, a) for a, b in up]),
        )
    done = []
    for _, dim in sides:
        low, high = edges[dim]
        around = [(width, width) if d in done else (0, 0) for d in range(array.ndim)]
        array = jnp.concatenate([jnp.pad(low, around), array, jnp.pad(high, around)], axis=dim)
        done.append(dim)
    return array


def extended_2(cells, sides, width):
    for axis, dim in sides:
        count = lax.axis_size(axis)
        head = lax.slice_in_dim(cells, 0, width, axis=dim)
        tail = lax.slice_in_dim(cells, cells.shape[dim] - width, cells.shape[dim], axis=dim)
        cells = jnp.concatenate(
            [
                lax.ppermute(tail, axis, [(i, (i + 1) % count) for i in range(count)]),
                cells,
                lax.ppermute(head, axis, [((i + 1) % count, i) for i in range(count)]),
            ],
            axis=dim,
        )
    return cells


def kernel_weight(offset):
    mag = jnp.abs(offset)
    inner = 1.0 - 2.5 * mag * mag + 1.5 * mag * mag * mag
    outer = 0.5 * (2.0 - mag) * (2.0 - mag) * (1.0 - mag)
    return jnp.where(mag < 1.0, inner, jnp.where(mag < 2.0, outer, 0.0 * mag))


def body(vorticity, wind):
    is_wake = lax.axis_index("grp") == 1
    velocity = spectral_velocity(vorticity, wind)[0]
    field = vorticity[0]
    count_x = field.shape[3]
    planes = shifted(velocity[..., count_x - 2 :], "grp", 1)
    rimmed = padded(velocity, (("gz", 1), ("gy", 2)), 1)
    grad_z = (rimmed[:, 2:, 1:-1, :] - rimmed[:, :-2, 1:-1, :]) * 0.5
    grad_y = (rimmed[:, 1:-1, 2:, :] - rimmed[:, 1:-1, :-2, :]) * 0.5
    left_side = jnp.where(is_wake, planes[..., 1:], velocity[..., count_x - 1 :])
    right_side = jnp.where(is_wake, velocity[..., count_x - 1 :], velocity[..., :1])
    extended = jnp.concatenate([left_side, velocity, right_side], -1)
    grad_x = (extended[..., 2:] - extended[..., :-2]) * 0.5
    strength = field + TIME_STEP * (field[0:1] * grad_x + field[1:2] * grad_y + field[2:3] * grad_z)
    ghost = shifted(strength[..., count_x - 2 :], "grp", 1)
    shift_x = TIME_STEP * velocity[0]
    left_q = jnp.where(is_wake, ghost, strength[..., count_x - 2 :])
    left_d = jnp.where(is_wake, TIME_STEP * planes[0], shift_x[..., count_x - 2 :])
    right_q = jnp.where(is_wake, 0.0, strength[..., :2])
    right_d = jnp.where(is_wake, 0.0, shift_x[..., :2])
    q_ext = jnp.concatenate([left_q, strength, right_q], -1)
    d_ext = jnp.concatenate([left_d, shift_x, right_d], -1)
    moved = jnp.zeros_like(strength)
    for offset in range(-2, 3):
        start = 2 - offset
        moved = moved + q_ext[..., start : start + count_x] * kernel_weight(
            offset - d_ext[..., start : start + count_x]
        )
    packed = jnp.concatenate([moved, TIME_STEP * velocity[1:2]], 0)
    rim_rows = extended_2(packed, (("gy", 2),), 2)
    width_y = moved.shape[2]
    lateral = jnp.zeros_like(moved)
    for offset in range(-2, 3):
        start = 2 - offset
        lateral = lateral + rim_rows[:3, :, start : start + width_y, :] * kernel_weight(
            offset - rim_rows[3:4, :, start : start + width_y, :]
        )
    packed = jnp.concatenate([lateral, TIME_STEP * velocity[2:3]], 0)
    rim_cols = extended_2(packed, (("gz", 1),), 2)
    width_z = moved.shape[1]
    result = jnp.zeros_like(moved)
    for offset in range(-2, 3):
        start = 2 - offset
        result = result + rim_cols[:3, start : start + width_z, :, :] * kernel_weight(
            offset - rim_cols[3:4, start : start + width_z, :, :]
        )
    return (result[None], velocity[None])


def solution(mesh):
    return jax.shard_map(
        body,
        mesh=mesh,
        in_specs=(P("grp", None, "gz", "gy", None), P("grp", None)),
        out_specs=(P("grp", None, "gz", "gy", None), P("grp", None, "gz", "gy", None)),
        check_vma=False,
    )
```

```python
import functools
import math

import jax
import jax.numpy as jnp
import numpy as np
from jax import lax
from jax.experimental import pallas as pl
from jax.experimental.pallas import tpu as pltpu
from jax.sharding import PartitionSpec as P

TIME_STEP = 0.4
MESH = pl.DeviceIdType.MESH
N = 256
HALF = 128
GY = 4
GZ = 32
PEERS = GY * GZ
LZ = 8
LY = 64


def split(values):
    high = values.astype(jnp.bfloat16)
    low = (values - high.astype(jnp.float32)).astype(jnp.bfloat16)
    return high, low


def table_pair(table):
    table = np.asarray(table, np.float32)
    high = table.astype(jnp.bfloat16)
    low = (table - high.astype(np.float32)).astype(jnp.bfloat16)
    return np.stack([high, low])


def make_tables():
    index = np.arange(N)
    angle = (index[:, None] * index[None, :] % N) * (2.0 * math.pi / N)
    cosine, sine = np.cos(angle), np.sin(angle)
    alternate = 1.0 - 2.0 * (index % 2)
    sine_in = -sine[:HALF].copy()
    sine_in[0] = alternate
    x_in = np.concatenate([cosine[:HALF], sine_in], 0)
    x_out = 2.0 * x_in / N
    x_out[0] *= 0.5
    x_out[HALF] *= 0.5
    cos_y = cosine.reshape(GY, 1, LY, N)
    sin_y = sine.reshape(GY, 1, LY, N)
    to_real = np.concatenate([cos_y, sin_y], 1).reshape(2 * N, N)
    to_imag = np.concatenate([-sin_y, cos_y], 1).reshape(2 * N, N)
    y_in = np.concatenate([to_real, to_imag], 1)
    y_out = np.concatenate([to_real, to_imag], 1).T / N
    z_all = np.stack([cosine, sine])
    return [table_pair(t) for t in (x_in, y_in, z_all, y_out, x_out)]


def dot3(a, b, dims=((1,), (0,))):
    def one(left, right):
        return lax.dot_general(left, right, (dims, ((), ())), preferred_element_type=jnp.float32)

    return one(a[0], b[0]) + (one(a[0], b[1]) + one(a[1], b[0]))


def each_peer(gy, gz, visit):
    for q in range(1, GY):
        visit(lax.rem(gy + q, GY), gz)

    def step(k, carry):
        other_z = lax.rem(gz + k, GZ)
        for q in range(GY):
            visit(lax.rem(gy + q, GY), other_z)
        return carry

    lax.fori_loop(1, GZ, step, 0)


def wait_bytes(ref, sem):
    pltpu.make_async_copy(ref, ref, sem).wait()


def waves(shape, axis):
    index = lax.broadcasted_iota(jnp.int32, shape, axis)
    signed = jnp.where(index < N // 2, index, index - N)
    full = signed.astype(jnp.float32) * (2.0 * math.pi / N)
    return full, jnp.where(index == N // 2, 0.0, full)


def kernel_weight(offset):
    mag = jnp.abs(offset)
    square = mag * mag
    inner = 1.0 + square * (1.5 * mag - 2.5)
    rest = 2.0 - mag
    outer = 0.5 * rest * rest * (1.0 - mag)
    return jnp.where(mag < 1.0, inner, jnp.where(mag < 2.0, outer, 0.0 * mag))


def moved_by(values, steps, axis):
    return pltpu.roll(values, steps % values.shape[axis], axis)


def step_kernel(
    field, wind, x_in, y_in, z_all, y_out, x_out, result_out, velocity_out,
    send, recv, stream, send2, recv2, scale, speed, weight_x, weight_y, weight_z,
    moved, result, row_out, row_in, column_out, column_in, ghost_out, ghost_in,
    lateral_out, lateral_in, layer_out, layer_in,
    ssem, rsem, ssem2, rsem2, plane_s, plane_r, row_s, row_r, column_s, column_r,
    ghost_s, ghost_r, lateral_s, lateral_r, layer_s, layer_r, store_s,
):
    grp = lax.axis_index("grp")
    gy = lax.axis_index("gy")
    gz = lax.axis_index("gz")
    me = gy * GZ + gz
    is_wake = grp == 1
    next_y, last_y = lax.rem(gy + 1, GY), lax.rem(gy + GY - 1, GY)
    next_z, last_z = lax.rem(gz + 1, GZ), lax.rem(gz + GZ - 1, GZ)
    barrier = pltpu.get_barrier_semaphore()

    def remote(source, target, sems, device):
        pltpu.make_async_remote_copy(
            source, target, sems[0], sems[1], device_id=device, device_id_type=MESH
        ).start()

    def greet(other_y, other_z):
        pl.semaphore_signal(
            barrier, inc=1, device_id={"gy": other_y, "gz": other_z}, device_id_type=MESH
        )

    each_peer(gy, gz, greet)
    pl.semaphore_signal(barrier, inc=1, device_id={"grp": 1 - grp}, device_id_type=MESH)

    lane = lax.broadcasted_iota(jnp.int32, (HALF, 128), 1)
    first_half = lane < LY
    for c in (1, 2, 0):
        for b in range(2):
            rows = field[0, c, 4 * b : 4 * b + 4].reshape(4 * LY, N)
            lines = dot3((x_in[0], x_in[1]), split(rows), ((1,), (1,)))
            for t in range(2):
                real = lines[:HALF, 128 * t : 128 * t + 128]
                imag = lines[HALF:, 128 * t : 128 * t + 128]
                even = jnp.where(first_half, real, pltpu.roll(imag, LY, 1))
                odd = jnp.where(first_half, pltpu.roll(real, LY, 1), imag)
                z = 4 * b + 2 * t
                send[c, pl.ds(z, HALF, stride=LZ), :] = even
                send[c, pl.ds(z + 1, HALF, stride=LZ), :] = odd
    mine = pl.ds(pl.multiple_of(me * LZ, LZ), LZ)
    mine_z = pl.ds(pl.multiple_of(gz * LZ, LZ), LZ)
    pl.semaphore_wait(barrier, PEERS)

    for c in (1, 2, 0):
        def out(other_y, other_z, c=c):
            other = other_y * GZ + other_z
            remote(
                send.at[c, pl.ds(pl.multiple_of(other * LZ, LZ), LZ)],
                recv.at[c, gy, mine_z],
                (ssem.at[c], rsem.at[c]),
                {"gy": other_y, "gz": other_z},
            )

        each_peer(gy, gz, out)
        recv[c, gy, mine_z, :] = send[c, mine, :]

    wave_z, curl_z = waves((N, N), 0)
    wave_y, curl_y = waves((N, N), 1)
    curl_x = me.astype(jnp.float32) * (2.0 * math.pi / N)
    squared = curl_x * curl_x + wave_y * wave_y + wave_z * wave_z
    positive = squared > 0
    scale[0] = jnp.where(positive, 1.0 / jnp.where(positive, squared, 1.0), 0.0)

    @pl.when(me == 0)
    def _():
        base = scale[0]
        top = 1.0 / (squared + math.pi * math.pi)
        scale[0] = 0.5 * (base + top)
        scale[1] = 0.5 * (base - top)

    curl = (curl_x, curl_y, curl_z)
    table_y = (y_in[0], y_in[1])
    cosine = (z_all[0, 0], z_all[1, 0])
    sine = (z_all[0, 1], z_all[1, 1])

    def transform(plane):
        lines = split(dot3(split(plane), table_y))
        by_cos = dot3(cosine, lines)
        by_sin = dot3(sine, lines)
        real = by_cos[:, :N] + by_sin[:, N:]
        imag = by_cos[:, N:] - by_sin[:, :N]
        return real, imag

    def forward(c):
        wait_bytes(recv2.at[c, pl.ds(0, (PEERS - 1) * LZ)], rsem.at[c])
        plane = jnp.concatenate([recv[c, j] for j in range(GY)], 1)
        real, imag = transform(plane)
        stream[c, 0] = real * scale[0]
        stream[c, 1] = imag * scale[0]

        @pl.when(me == 0)
        def _():
            column = lax.broadcasted_iota(jnp.int32, (N, 2 * N), 1)
            plane = jnp.concatenate([recv[c, j] for j in range(GY)], 1)
            real, imag = transform(jnp.where(column % 128 < LY, plane, -plane))
            stream[c, 0] += real * scale[1]
            stream[c, 1] += imag * scale[1]

    def backward(d):
        a, b = (d + 1) % 3, (d + 2) % 3
        real = curl[b] * stream[a, 1] - curl[a] * stream[b, 1]
        imag = curl[a] * stream[b, 0] - curl[b] * stream[a, 0]
        lines = split(jnp.concatenate([real, imag], 1))
        by_cos = dot3(cosine, lines)
        by_sin = dot3(sine, lines)
        real = by_cos[:, :N] - by_sin[:, N:]
        imag = by_cos[:, N:] + by_sin[:, :N]
        lines = split(jnp.concatenate([real, imag], 1) * (1.0 / N))
        plane = dot3(lines, (y_out[0], y_out[1]))
        for j in range(GY):
            send2[d, j] = plane[:, 128 * j : 128 * j + 128]

        def out(other_y, other_z):
            remote(
                send2.at[d, other_y, pl.ds(pl.multiple_of(other_z * LZ, LZ), LZ)],
                recv2.at[d, mine],
                (ssem2.at[d], rsem2.at[d]),
                {"gy": other_y, "gz": other_z},
            )

        each_peer(gy, gz, out)
        recv2[d, mine, :] = send2[d, gy, mine_z, :]

    forward(1)
    forward(2)
    backward(0)
    forward(0)
    backward(1)
    backward(2)

    row = lax.broadcasted_iota(jnp.int32, (LY, N), 0)
    column = lax.broadcasted_iota(jnp.int32, (LY, N), 1)
    tile = lax.broadcasted_iota(jnp.int32, (LY, 128), 1)
    short_row = lax.broadcasted_iota(jnp.int32, (8, N), 0)
    no_wrap_low = jnp.where(is_wake, 0, -N)
    no_wrap_high = jnp.where(is_wake, N, 2 * N)
    first_column = jnp.where(is_wake, 0, -1)
    last_column = jnp.where(is_wake, N - 1, N)

    def velocity_of(d):
        wait_bytes(recv.at[0, :, pl.ds(0, (PEERS - 1) * LZ // GY)], rsem2.at[d])
        drift = wind[0, d]
        edge = jnp.zeros((LY, 128), jnp.float32)
        for b in range(2):
            parts = []
            for z in range(4 * b, 4 * b + 4):
                turned = recv2[d, pl.ds(z, HALF, stride=LZ), :].T
                parts.append(jnp.concatenate([turned[:LY], turned[LY:]], 1))
            lines = split(jnp.concatenate(parts, 0))
            out = dot3(lines, (x_out[0], x_out[1])) + drift
            for z in range(4 * b, 4 * b + 4):
                plane = out[LY * (z - 4 * b) : LY * (z - 4 * b) + LY]
                speed[d, z + 1] = plane
                row_out[0, d * LZ + z : d * LZ + z + 1, :] = plane[LY - 1 :]
                row_out[1, d * LZ + z : d * LZ + z + 1, :] = plane[:1]
                edge = jnp.where(tile == z, pltpu.roll(plane[:, 128:], z + 1, 1), edge)
        column_out[d] = edge
        rows = pl.ds(d * LZ, LZ)
        remote(speed.at[d, LZ], speed.at[d, 0], (plane_s.at[d], plane_r.at[d]), {"gz": next_z})
        remote(speed.at[d, 1], speed.at[d, LZ + 1], (plane_s.at[d], plane_r.at[d]), {"gz": last_z})
        remote(row_out.at[0, rows], row_in.at[0, rows], (row_s.at[d], row_r.at[d]), {"gy": next_y})
        remote(row_out.at[1, rows], row_in.at[1, rows], (row_s.at[d], row_r.at[d]), {"gy": last_y})

        @pl.when(grp == 0)
        def _():
            remote(column_out.at[d], column_in.at[d], (column_s.at[d], column_r.at[d]), {"grp": 1})

        pltpu.make_async_copy(
            speed.at[d, pl.ds(1, LZ)], velocity_out.at[0, d], store_s.at[d]
        ).start()

    def weights(target, d):
        def at(z, carry):
            shift = TIME_STEP * speed[d, z + 1]
            for offset in range(-2, 3):
                value = kernel_weight(offset - shift)
                if d == 0 and offset > 0:
                    value = jnp.where(column >= no_wrap_high - offset, 0.0, value)
                if d == 0 and offset < 0:
                    value = jnp.where(column < no_wrap_low - offset, 0.0, value)
                target[offset + 2, z] = value
            return carry

        lax.fori_loop(0, LZ, at, 0)

    def stretch(d):
        wait_bytes(speed.at[d, pl.ds(0, 2)], plane_r.at[d])
        wait_bytes(row_in.at[0, pl.ds(0, 2 * LZ)], row_r.at[d])

        @pl.when(is_wake)
        def _():
            wait_bytes(column_in.at[d], column_r.at[d])

        def at(z, ghost):
            here = speed[d, z + 1]
            grad_z = speed[d, z + 2] - speed[d, z]
            low = row_in[0, pl.ds(d * LZ + z, 1), :]
            high = row_in[1, pl.ds(d * LZ + z, 1), :]
            up = jnp.where(row == LY - 1, high, moved_by(here, -1, 0))
            down = jnp.where(row == 0, low, moved_by(here, 1, 0))
            inflow = pltpu.roll(column_in[d], lax.rem(128 - z, 128), 1)
            left = moved_by(here, 1, 1)
            left = jnp.concatenate(
                [jnp.where(tile == first_column, inflow, left[:, :128]), left[:, 128:]], 1
            )
            right = jnp.where(column == last_column, here, moved_by(here, -1, 1))
            strength = field[0, d, z] + (0.5 * TIME_STEP) * (
                field[0, 0, z] * (right - left)
                + field[0, 1, z] * (up - down)
                + field[0, 2, z] * grad_z
            )
            one = moved_by(strength * weight_x[3, z], 1, 1)
            two = moved_by(strength * weight_x[4, z], 2, 1)
            total = strength * weight_x[2, z] + one + two
            total = total + moved_by(strength * weight_x[1, z], -1, 1)
            moved[d, z] = total + moved_by(strength * weight_x[0, z], -2, 1)
            over = jnp.where(tile == 0, one[:, :128], 0.0) + jnp.where(tile < 2, two[:, :128], 0.0)
            return ghost + pltpu.roll(over, 2 * z, 1)

        ghost_out[d] = lax.fori_loop(0, LZ, at, jnp.zeros((LY, 128), jnp.float32))

        @pl.when(grp == 0)
        def _():
            remote(ghost_out.at[d], ghost_in.at[d], (ghost_s.at[d], ghost_r.at[d]), {"grp": 1})

    def lateral_send(d):
        @pl.when(is_wake)
        def _():
            wait_bytes(ghost_in.at[d], ghost_r.at[d])

            def add(z, carry):
                inflow = pltpu.roll(ghost_in[d], lax.rem(128 - 2 * z, 128), 1)
                moved[d, z, :, :128] += jnp.where(tile < 2, inflow, 0.0)
                return carry

            lax.fori_loop(0, LZ, add, 0)

        def at(z, carry):
            here = moved[d, z]
            one = moved_by(here * weight_y[3, z], 1, 0)
            two = moved_by(here * weight_y[4, z], 2, 0)
            back_one = moved_by(here * weight_y[1, z], -1, 0)
            back_two = moved_by(here * weight_y[0, z], -2, 0)
            total = here * weight_y[2, z]
            total = total + jnp.where(row < 1, 0.0, one) + jnp.where(row < 2, 0.0, two)
            total = total + jnp.where(row >= LY - 1, 0.0, back_one)
            moved[d, z] = total + jnp.where(row >= LY - 2, 0.0, back_two)
            at_z = pl.ds(d * LZ + z, 1)
            lateral_out[0, 0, at_z, :] = one[0:1] + two[0:1]
            lateral_out[0, 1, at_z, :] = two[1:2]
            lateral_out[1, 0, at_z, :] = back_two[LY - 2 : LY - 1]
            lateral_out[1, 1, at_z, :] = back_one[LY - 1 :] + back_two[LY - 1 :]
            return carry

        lax.fori_loop(0, LZ, at, 0)
        rows = pl.ds(d * LZ, LZ)
        for side, other in ((0, next_y), (1, last_y)):
            for step in range(2):
                remote(
                    lateral_out.at[side, step, rows],
                    lateral_in.at[side, step, rows],
                    (lateral_s.at[d], lateral_r.at[d]),
                    {"gy": other},
                )

    def layers_send(d):
        wait_bytes(row_in.at[:, pl.ds(0, 2 * LZ)], lateral_r.at[d])

        def add(z, carry):
            at_z = pl.ds(d * LZ + z, 1)
            first, second = lateral_in[0, 0, at_z, :], lateral_in[0, 1, at_z, :]
            third, fourth = lateral_in[1, 0, at_z, :], lateral_in[1, 1, at_z, :]
            moved[d, z, :8] += jnp.where(
                short_row == 0, first, jnp.where(short_row == 1, second, 0.0)
            )
            moved[d, z, LY - 8 :] += jnp.where(
                short_row == 6, third, jnp.where(short_row == 7, fourth, 0.0)
            )
            return carry

        lax.fori_loop(0, LZ, add, 0)
        end = LZ - 1
        layer_out[0, d, 0] = moved[d, end] * weight_z[3, end] + moved[d, end - 1] * weight_z[4, end - 1]
        layer_out[0, d, 1] = moved[d, end] * weight_z[4, end]
        layer_out[1, d, 0] = moved[d, 0] * weight_z[0, 0]
        layer_out[1, d, 1] = moved[d, 0] * weight_z[1, 0] + moved[d, 1] * weight_z[0, 1]
        for side, other in ((0, next_z), (1, last_z)):
            remote(
                layer_out.at[side, d],
                layer_in.at[side, d],
                (layer_s.at[d], layer_r.at[d]),
                {"gz": other},
            )
        for z in range(LZ):
            total = moved[d, z] * weight_z[2, z]
            for offset in (-2, -1, 1, 2):
                if 0 <= z - offset < LZ:
                    total = total + moved[d, z - offset] * weight_z[offset + 2, z - offset]
            result[d, z] = total

    def finish(d):
        wait_bytes(layer_in.at[:, d], layer_r.at[d])
        for side, start in ((0, 0), (1, LZ - 2)):
            for step in range(2):
                result[d, start + step] += layer_in[side, d, step]
        pltpu.make_async_copy(result.at[d], result_out.at[0, d], store_s.at[3 + d]).start()

    velocity_of(0)
    weights(weight_x, 0)
    stretch(0)
    velocity_of(1)
    weights(weight_y, 1)
    lateral_send(0)
    stretch(1)
    velocity_of(2)
    weights(weight_z, 2)
    layers_send(0)
    lateral_send(1)
    stretch(2)
    layers_send(1)
    finish(0)
    lateral_send(2)
    layers_send(2)
    finish(1)
    finish(2)

    for c in range(3):
        wait_bytes(send.at[c, pl.ds(0, (PEERS - 1) * LZ)], ssem.at[c])
        wait_bytes(send.at[c, pl.ds(0, (PEERS - 1) * LZ)], ssem2.at[c])
        wait_bytes(speed.at[c, pl.ds(0, 2)], plane_s.at[c])
        wait_bytes(row_out.at[0, pl.ds(0, 2 * LZ)], row_s.at[c])
        wait_bytes(row_out.at[:, pl.ds(0, 2 * LZ)], lateral_s.at[c])
        wait_bytes(layer_out.at[:, c], layer_s.at[c])
        wait_bytes(result.at[c], store_s.at[c])
        wait_bytes(result.at[c], store_s.at[3 + c])

        @pl.when(grp == 0)
        def _():
            wait_bytes(column_out.at[c], column_s.at[c])
            wait_bytes(ghost_out.at[c], ghost_s.at[c])


def body(vorticity, wind):
    tables = [jnp.asarray(t) for t in make_tables()]
    vmem = pl.BlockSpec(memory_space=pltpu.VMEM)
    shape = jax.ShapeDtypeStruct(vorticity.shape, jnp.float32)
    block = (3, LZ, LY, N)
    buffers = [
        (3, PEERS * LZ, 128),
        (3, GY, N, 128),
        (3, 2, N, N),
        (3, GY, N, 128),
        (3, PEERS * LZ, 128),
        (2, N, N),
        (3, LZ + 2, LY, N),
        (5, LZ, LY, N),
        (5, LZ, LY, N),
        (5, LZ, LY, N),
        block,
        block,
        (2, 3 * LZ, N),
        (2, 3 * LZ, N),
        (3, LY, 128),
        (3, LY, 128),
        (3, LY, 128),
        (3, LY, 128),
        (2, 2, 3 * LZ, N),
        (2, 2, 3 * LZ, N),
        (2, 3, 2, LY, N),
        (2, 3, 2, LY, N),
    ]
    result, velocity = pl.pallas_call(
        step_kernel,
        out_shape=(shape, shape),
        in_specs=[vmem, pl.BlockSpec(memory_space=pltpu.SMEM)] + [vmem] * 5,
        out_specs=(pl.BlockSpec(memory_space=pl.ANY), pl.BlockSpec(memory_space=pl.ANY)),
        scratch_shapes=[pltpu.VMEM(b, jnp.float32) for b in buffers]
        + [pltpu.SemaphoreType.DMA((3,))] * 16
        + [pltpu.SemaphoreType.DMA((6,))],
        compiler_params=pltpu.CompilerParams(collective_id=0, has_side_effects=True),
    )(vorticity, wind, *tables)
    return result, velocity


def solution(mesh):
    return jax.shard_map(
        body,
        mesh=mesh,
        in_specs=(P("grp", None, "gz", "gy", None), P("grp", None)),
        out_specs=(P("grp", None, "gz", "gy", None), P("grp", None, "gz", "gy", None)),
        check_vma=False,
    )
```

```python
import functools
import math

import jax
import jax.numpy as jnp
import numpy as np
from jax import lax
from jax.experimental import pallas as pl
from jax.experimental.pallas import tpu as pltpu
from jax.sharding import PartitionSpec as P

TIME_STEP = 0.4
MESH = pl.DeviceIdType.MESH
N = 256
HALF = 128
GY = 4
GZ = 32
PEERS = GY * GZ
LZ = 8
LY = 64


def split(values):
    high = values.astype(jnp.bfloat16)
    low = (values - high.astype(jnp.float32)).astype(jnp.bfloat16)
    return high, low


def table_pair(table):
    table = np.asarray(table, np.float32)
    high = table.astype(jnp.bfloat16)
    low = (table - high.astype(np.float32)).astype(jnp.bfloat16)
    return np.stack([high, low])


def make_tables():
    index = np.arange(N)
    angle = (index[:, None] * index[None, :] % N) * (2.0 * math.pi / N)
    cosine, sine = np.cos(angle), np.sin(angle)
    alternate = 1.0 - 2.0 * (index % 2)
    sine_in = -sine[:HALF].copy()
    sine_in[0] = alternate
    x_in = np.concatenate([cosine[:HALF], sine_in], 0)
    x_out = 2.0 * x_in / N
    x_out[0] *= 0.5
    x_out[HALF] *= 0.5
    cos_y = cosine.reshape(GY, 1, LY, N)
    sin_y = sine.reshape(GY, 1, LY, N)
    to_real = np.concatenate([cos_y, sin_y], 1).reshape(2 * N, N)
    to_imag = np.concatenate([-sin_y, cos_y], 1).reshape(2 * N, N)
    y_in = np.concatenate([to_real, to_imag], 1)
    y_out = np.concatenate([to_real, to_imag], 1).T / N
    z_all = np.stack([cosine, sine])
    return [table_pair(t) for t in (x_in, y_in, z_all, y_out, x_out)]


def dot3(a, b, dims=((1,), (0,))):
    def one(left, right):
        return lax.dot_general(left, right, (dims, ((), ())), preferred_element_type=jnp.float32)

    return one(a[0], b[0]) + (one(a[0], b[1]) + one(a[1], b[0]))


def each_peer(gy, gz, visit):
    for q in range(1, GY):
        visit(lax.rem(gy + q, GY), gz)

    def step(k, carry):
        other_z = lax.rem(gz + k, GZ)
        for q in range(GY):
            visit(lax.rem(gy + q, GY), other_z)
        return carry

    lax.fori_loop(1, GZ, step, 0)


def wait_bytes(ref, sem):
    pltpu.make_async_copy(ref, ref, sem).wait()


def waves(shape, axis):
    index = lax.broadcasted_iota(jnp.int32, shape, axis)
    signed = jnp.where(index < N // 2, index, index - N)
    full = signed.astype(jnp.float32) * (2.0 * math.pi / N)
    return full, jnp.where(index == N // 2, 0.0, full)


def kernel_weight(offset):
    mag = jnp.abs(offset)
    square = mag * mag
    inner = 1.0 + square * (1.5 * mag - 2.5)
    rest = 2.0 - mag
    outer = 0.5 * rest * rest * (1.0 - mag)
    return jnp.where(mag < 1.0, inner, jnp.where(mag < 2.0, outer, 0.0 * mag))


def moved_by(values, steps, axis):
    return pltpu.roll(values, steps % values.shape[axis], axis)


def step_kernel(
    field_in, wind, x_in_h, y_in_h, z_all_h, y_out_h, x_out_h, result, speed,
    field, x_in, y_in, z_all, y_out, x_out, send, recv, stream, send2, recv2, scale, weight_x, weight_y, weight_z,
    moved, row_out, row_in, column_out, column_in, ghost_out, ghost_in,
    lateral_out, lateral_in, layer_out, layer_in,
    ssem, rsem, ssem2, rsem2, plane_s, plane_r, row_s, row_r, column_s, column_r,
    ghost_s, ghost_r, lateral_s, lateral_r, layer_s, layer_r, load_s,
):
    grp = lax.axis_index("grp")
    gy = lax.axis_index("gy")
    gz = lax.axis_index("gz")
    me = gy * GZ + gz
    is_wake = grp == 1
    next_y, last_y = lax.rem(gy + 1, GY), lax.rem(gy + GY - 1, GY)
    next_z, last_z = lax.rem(gz + 1, GZ), lax.rem(gz + GZ - 1, GZ)
    barrier = pltpu.get_barrier_semaphore()

    def remote(source, target, sems, device):
        pltpu.make_async_remote_copy(
            source, target, sems[0], sems[1], device_id=device, device_id_type=MESH
        ).start()

    def greet(other_y, other_z):
        pl.semaphore_signal(
            barrier, inc=1, device_id={"gy": other_y, "gz": other_z}, device_id_type=MESH
        )

    def load(source, target, index):
        pltpu.make_async_copy(source, target, load_s.at[index]).start()

    load(x_in_h, x_in, 3)
    for c in (1, 2, 0):
        load(field_in.at[0, c], field.at[0, c], c)
    load(y_in_h, y_in, 4)
    load(z_all_h, z_all, 5)
    load(y_out_h, y_out, 6)
    load(x_out_h, x_out, 7)
    each_peer(gy, gz, greet)
    pl.semaphore_signal(barrier, inc=1, device_id={"grp": 1 - grp}, device_id_type=MESH)

    lane = lax.broadcasted_iota(jnp.int32, (HALF, 128), 1)
    first_half = lane < LY
    wait_bytes(x_in, load_s.at[3])
    for c in (1, 2, 0):
        wait_bytes(field.at[0, c], load_s.at[c])
        for b in range(2):
            rows = field[0, c, 4 * b : 4 * b + 4].reshape(4 * LY, N)
            lines = dot3((x_in[0], x_in[1]), split(rows), ((1,), (1,)))
            for t in range(2):
                real = lines[:HALF, 128 * t : 128 * t + 128]
                imag = lines[HALF:, 128 * t : 128 * t + 128]
                even = jnp.where(first_half, real, pltpu.roll(imag, LY, 1))
                odd = jnp.where(first_half, pltpu.roll(real, LY, 1), imag)
                z = 4 * b + 2 * t
                send[c, pl.ds(z, HALF, stride=LZ), :] = even
                send[c, pl.ds(z + 1, HALF, stride=LZ), :] = odd
    mine = pl.ds(pl.multiple_of(me * LZ, LZ), LZ)
    mine_z = pl.ds(pl.multiple_of(gz * LZ, LZ), LZ)
    pl.semaphore_wait(barrier, PEERS)

    for c in (1, 2, 0):
        def out(other_y, other_z, c=c):
            other = other_y * GZ + other_z
            remote(
                send.at[c, pl.ds(pl.multiple_of(other * LZ, LZ), LZ)],
                recv.at[c, gy, mine_z],
                (ssem.at[c], rsem.at[c]),
                {"gy": other_y, "gz": other_z},
            )

        each_peer(gy, gz, out)
        recv[c, gy, mine_z, :] = send[c, mine, :]

    wave_z, curl_z = waves((N, N), 0)
    wave_y, curl_y = waves((N, N), 1)
    curl_x = me.astype(jnp.float32) * (2.0 * math.pi / N)
    squared = curl_x * curl_x + wave_y * wave_y + wave_z * wave_z
    positive = squared > 0
    scale[0] = jnp.where(positive, 1.0 / jnp.where(positive, squared, 1.0), 0.0)

    @pl.when(me == 0)
    def _():
        base = scale[0]
        top = 1.0 / (squared + math.pi * math.pi)
        scale[0] = 0.5 * (base + top)
        scale[1] = 0.5 * (base - top)

    wait_bytes(y_in, load_s.at[4])
    wait_bytes(z_all, load_s.at[5])
    wait_bytes(y_out, load_s.at[6])
    wait_bytes(x_out, load_s.at[7])
    curl = (curl_x, curl_y, curl_z)
    table_y = (y_in[0], y_in[1])
    cosine = (z_all[0, 0], z_all[1, 0])
    sine = (z_all[0, 1], z_all[1, 1])

    def transform(plane):
        lines = split(dot3(split(plane), table_y))
        by_cos = dot3(cosine, lines)
        by_sin = dot3(sine, lines)
        real = by_cos[:, :N] + by_sin[:, N:]
        imag = by_cos[:, N:] - by_sin[:, :N]
        return real, imag

    def forward(c):
        wait_bytes(recv2.at[c, pl.ds(0, (PEERS - 1) * LZ)], rsem.at[c])
        plane = jnp.concatenate([recv[c, j] for j in range(GY)], 1)
        real, imag = transform(plane)
        stream[c, 0] = real * scale[0]
        stream[c, 1] = imag * scale[0]

        @pl.when(me == 0)
        def _():
            column = lax.broadcasted_iota(jnp.int32, (N, 2 * N), 1)
            plane = jnp.concatenate([recv[c, j] for j in range(GY)], 1)
            real, imag = transform(jnp.where(column % 128 < LY, plane, -plane))
            stream[c, 0] += real * scale[1]
            stream[c, 1] += imag * scale[1]

    def backward(d):
        a, b = (d + 1) % 3, (d + 2) % 3
        real = curl[b] * stream[a, 1] - curl[a] * stream[b, 1]
        imag = curl[a] * stream[b, 0] - curl[b] * stream[a, 0]
        lines = split(jnp.concatenate([real, imag], 1))
        by_cos = dot3(cosine, lines)
        by_sin = dot3(sine, lines)
        real = by_cos[:, :N] - by_sin[:, N:]
        imag = by_cos[:, N:] + by_sin[:, :N]
        lines = split(jnp.concatenate([real, imag], 1) * (1.0 / N))
        plane = dot3(lines, (y_out[0], y_out[1]))
        for j in range(GY):
            send2[d, j] = plane[:, 128 * j : 128 * j + 128]

    def send_back(d):
        def out(other_y, other_z):
            remote(
                send2.at[d, other_y, pl.ds(pl.multiple_of(other_z * LZ, LZ), LZ)],
                recv2.at[d, mine],
                (ssem2.at[d], rsem2.at[d]),
                {"gy": other_y, "gz": other_z},
            )

        each_peer(gy, gz, out)
        recv2[d, mine, :] = send2[d, gy, mine_z, :]

    forward(1)
    forward(2)
    backward(0)
    send_back(0)
    forward(0)
    backward(1)
    send_back(1)
    backward(2)

    row = lax.broadcasted_iota(jnp.int32, (LY, N), 0)
    column = lax.broadcasted_iota(jnp.int32, (LY, N), 1)
    tile = lax.broadcasted_iota(jnp.int32, (LY, 128), 1)
    short_row = lax.broadcasted_iota(jnp.int32, (8, N), 0)
    no_wrap_low = jnp.where(is_wake, 0, -N)
    no_wrap_high = jnp.where(is_wake, N, 2 * N)
    first_column = jnp.where(is_wake, 0, -1)
    last_column = jnp.where(is_wake, N - 1, N)

    def velocity_of(d):
        wait_bytes(recv.at[0, :, pl.ds(0, (PEERS - 1) * LZ // GY)], rsem2.at[d])
        drift = wind[0, d]
        edge = jnp.zeros((LY, 128), jnp.float32)
        for b in range(2):
            parts = []
            for z in range(4 * b, 4 * b + 4):
                turned = recv2[d, pl.ds(z, HALF, stride=LZ), :].T
                parts.append(jnp.concatenate([turned[:LY], turned[LY:]], 1))
            lines = split(jnp.concatenate(parts, 0))
            out = dot3(lines, (x_out[0], x_out[1])) + drift
            for z in range(4 * b, 4 * b + 4):
                plane = out[LY * (z - 4 * b) : LY * (z - 4 * b) + LY]
                speed[d, z + 1] = plane
                row_out[0, d * LZ + z : d * LZ + z + 1, :] = plane[LY - 1 :]
                row_out[1, d * LZ + z : d * LZ + z + 1, :] = plane[:1]
                edge = jnp.where(tile == z, pltpu.roll(plane[:, 128:], z + 1, 1), edge)
        column_out[d] = edge
        rows = pl.ds(d * LZ, LZ)
        remote(speed.at[d, LZ], speed.at[d, 0], (plane_s.at[d], plane_r.at[d]), {"gz": next_z})
        remote(speed.at[d, 1], speed.at[d, LZ + 1], (plane_s.at[d], plane_r.at[d]), {"gz": last_z})
        remote(row_out.at[0, rows], row_in.at[0, rows], (row_s.at[d], row_r.at[d]), {"gy": next_y})
        remote(row_out.at[1, rows], row_in.at[1, rows], (row_s.at[d], row_r.at[d]), {"gy": last_y})

        @pl.when(grp == 0)
        def _():
            remote(column_out.at[d], column_in.at[d], (column_s.at[d], column_r.at[d]), {"grp": 1})

    def weights(target, d):
        def at(z, carry):
            shift = TIME_STEP * speed[d, z + 1]
            for offset in range(-2, 3):
                value = kernel_weight(offset - shift)
                if d == 0 and offset > 0:
                    value = jnp.where(column >= no_wrap_high - offset, 0.0, value)
                if d == 0 and offset < 0:
                    value = jnp.where(column < no_wrap_low - offset, 0.0, value)
                target[offset + 2, z] = value
            return carry

        lax.fori_loop(0, LZ, at, 0)

    def stretch(d):
        wait_bytes(speed.at[d, pl.ds(0, 2)], plane_r.at[d])
        wait_bytes(row_in.at[0, pl.ds(0, 2 * LZ)], row_r.at[d])

        @pl.when(is_wake)
        def _():
            wait_bytes(column_in.at[d], column_r.at[d])

        def at(z, ghost):
            here = speed[d, z + 1]
            grad_z = speed[d, z + 2] - speed[d, z]
            low = row_in[0, pl.ds(d * LZ + z, 1), :]
            high = row_in[1, pl.ds(d * LZ + z, 1), :]
            up = jnp.where(row == LY - 1, high, moved_by(here, -1, 0))
            down = jnp.where(row == 0, low, moved_by(here, 1, 0))
            inflow = pltpu.roll(column_in[d], lax.rem(128 - z, 128), 1)
            left = moved_by(here, 1, 1)
            left = jnp.concatenate(
                [jnp.where(tile == first_column, inflow, left[:, :128]), left[:, 128:]], 1
            )
            right = jnp.where(column == last_column, here, moved_by(here, -1, 1))
            strength = field[0, d, z] + (0.5 * TIME_STEP) * (
                field[0, 0, z] * (right - left)
                + field[0, 1, z] * (up - down)
                + field[0, 2, z] * grad_z
            )
            one = moved_by(strength * weight_x[3, z], 1, 1)
            two = moved_by(strength * weight_x[4, z], 2, 1)
            total = strength * weight_x[2, z] + one + two
            total = total + moved_by(strength * weight_x[1, z], -1, 1)
            moved[d, z] = total + moved_by(strength * weight_x[0, z], -2, 1)
            over = jnp.where(tile == 0, one[:, :128], 0.0) + jnp.where(tile < 2, two[:, :128], 0.0)
            return ghost + pltpu.roll(over, 2 * z, 1)

        ghost_out[d] = lax.fori_loop(0, LZ, at, jnp.zeros((LY, 128), jnp.float32))

        @pl.when(grp == 0)
        def _():
            remote(ghost_out.at[d], ghost_in.at[d], (ghost_s.at[d], ghost_r.at[d]), {"grp": 1})

    def lateral_send(d):
        @pl.when(is_wake)
        def _():
            wait_bytes(ghost_in.at[d], ghost_r.at[d])

            def add(z, carry):
                inflow = pltpu.roll(ghost_in[d], lax.rem(128 - 2 * z, 128), 1)
                moved[d, z, :, :128] += jnp.where(tile < 2, inflow, 0.0)
                return carry

            lax.fori_loop(0, LZ, add, 0)

        def at(z, carry):
            here = moved[d, z]
            one = moved_by(here * weight_y[3, z], 1, 0)
            two = moved_by(here * weight_y[4, z], 2, 0)
            back_one = moved_by(here * weight_y[1, z], -1, 0)
            back_two = moved_by(here * weight_y[0, z], -2, 0)
            total = here * weight_y[2, z]
            total = total + jnp.where(row < 1, 0.0, one) + jnp.where(row < 2, 0.0, two)
            total = total + jnp.where(row >= LY - 1, 0.0, back_one)
            moved[d, z] = total + jnp.where(row >= LY - 2, 0.0, back_two)
            at_z = pl.ds(d * LZ + z, 1)
            lateral_out[0, 0, at_z, :] = one[0:1] + two[0:1]
            lateral_out[0, 1, at_z, :] = two[1:2]
            lateral_out[1, 0, at_z, :] = back_two[LY - 2 : LY - 1]
            lateral_out[1, 1, at_z, :] = back_one[LY - 1 :] + back_two[LY - 1 :]
            return carry

        lax.fori_loop(0, LZ, at, 0)
        rows = pl.ds(d * LZ, LZ)
        for side, other in ((0, next_y), (1, last_y)):
            for step in range(2):
                remote(
                    lateral_out.at[side, step, rows],
                    lateral_in.at[side, step, rows],
                    (lateral_s.at[d], lateral_r.at[d]),
                    {"gy": other},
                )

    def layers_send(d):
        wait_bytes(row_in.at[:, pl.ds(0, 2 * LZ)], lateral_r.at[d])

        def add(z, carry):
            at_z = pl.ds(d * LZ + z, 1)
            first, second = lateral_in[0, 0, at_z, :], lateral_in[0, 1, at_z, :]
            third, fourth = lateral_in[1, 0, at_z, :], lateral_in[1, 1, at_z, :]
            moved[d, z, :8] += jnp.where(
                short_row == 0, first, jnp.where(short_row == 1, second, 0.0)
            )
            moved[d, z, LY - 8 :] += jnp.where(
                short_row == 6, third, jnp.where(short_row == 7, fourth, 0.0)
            )
            return carry

        lax.fori_loop(0, LZ, add, 0)
        end = LZ - 1
        layer_out[0, d, 0] = moved[d, end] * weight_z[3, end] + moved[d, end - 1] * weight_z[4, end - 1]
        layer_out[0, d, 1] = moved[d, end] * weight_z[4, end]
        layer_out[1, d, 0] = moved[d, 0] * weight_z[0, 0]
        layer_out[1, d, 1] = moved[d, 0] * weight_z[1, 0] + moved[d, 1] * weight_z[0, 1]
        for side, other in ((0, next_z), (1, last_z)):
            remote(
                layer_out.at[side, d],
                layer_in.at[side, d],
                (layer_s.at[d], layer_r.at[d]),
                {"gz": other},
            )
        for z in range(LZ):
            total = moved[d, z] * weight_z[2, z]
            for offset in (-2, -1, 1, 2):
                if 0 <= z - offset < LZ:
                    total = total + moved[d, z - offset] * weight_z[offset + 2, z - offset]
            result[d, z] = total

    def finish(d):
        wait_bytes(layer_in.at[:, d], layer_r.at[d])
        for side, start in ((0, 0), (1, LZ - 2)):
            for step in range(2):
                result[d, start + step] += layer_in[side, d, step]

    velocity_of(0)
    send_back(2)
    weights(weight_x, 0)
    stretch(0)
    velocity_of(1)
    weights(weight_y, 1)
    lateral_send(0)
    stretch(1)
    velocity_of(2)
    weights(weight_z, 2)
    layers_send(0)
    lateral_send(1)
    stretch(2)
    layers_send(1)
    finish(0)
    lateral_send(2)
    layers_send(2)
    finish(1)
    finish(2)

    for c in range(3):
        wait_bytes(send.at[c, pl.ds(0, (PEERS - 1) * LZ)], ssem.at[c])
        wait_bytes(send.at[c, pl.ds(0, (PEERS - 1) * LZ)], ssem2.at[c])
        wait_bytes(speed.at[c, pl.ds(0, 2)], plane_s.at[c])
        wait_bytes(row_out.at[0, pl.ds(0, 2 * LZ)], row_s.at[c])
        wait_bytes(row_out.at[:, pl.ds(0, 2 * LZ)], lateral_s.at[c])
        wait_bytes(layer_out.at[:, c], layer_s.at[c])

        @pl.when(grp == 0)
        def _():
            wait_bytes(column_out.at[c], column_s.at[c])
            wait_bytes(ghost_out.at[c], ghost_s.at[c])


def output_kernel(result, speed, result_out, velocity_out, sems):
    copies = [
        pltpu.make_async_copy(speed.at[:, pl.ds(1, LZ)], velocity_out.at[0], sems.at[0]),
        pltpu.make_async_copy(result, result_out.at[0], sems.at[1]),
    ]
    for copy in copies:
        copy.start()
    for copy in copies:
        copy.wait()


def body(vorticity, wind):
    tables = [jnp.asarray(t) for t in make_tables()]
    anywhere = pl.BlockSpec(memory_space=pl.ANY)
    near = pl.BlockSpec(memory_space=pltpu.VMEM)
    shape = jax.ShapeDtypeStruct(vorticity.shape, jnp.float32)
    block = (3, LZ, LY, N)
    buffers = [
        (3, PEERS * LZ, 128),
        (3, GY, N, 128),
        (3, 2, N, N),
        (3, GY, N, 128),
        (3, PEERS * LZ, 128),
        (2, N, N),
        (5, LZ, LY, N),
        (5, LZ, LY, N),
        (5, LZ, LY, N),
        block,
        (2, 3 * LZ, N),
        (2, 3 * LZ, N),
        (3, LY, 128),
        (3, LY, 128),
        (3, LY, 128),
        (3, LY, 128),
        (2, 2, 3 * LZ, N),
        (2, 2, 3 * LZ, N),
        (2, 3, 2, LY, N),
        (2, 3, 2, LY, N),
    ]
    result, speed = pl.pallas_call(
        step_kernel,
        out_shape=(pltpu.VMEM(block, jnp.float32), pltpu.VMEM((3, LZ + 2, LY, N), jnp.float32)),
        in_specs=[anywhere, pl.BlockSpec(memory_space=pltpu.SMEM)] + [anywhere] * 5,
        out_specs=(pl.BlockSpec(memory_space=pltpu.VMEM), pl.BlockSpec(memory_space=pltpu.VMEM)),
        scratch_shapes=[pltpu.VMEM(vorticity.shape, jnp.float32)]
        + [pltpu.VMEM(t.shape, jnp.bfloat16) for t in tables]
        + [pltpu.VMEM(b, jnp.float32) for b in buffers]
        + [pltpu.SemaphoreType.DMA((3,))] * 16
        + [pltpu.SemaphoreType.DMA((8,))],
        compiler_params=pltpu.CompilerParams(collective_id=0, has_side_effects=True),
    )(vorticity, wind, *tables)
    return pl.pallas_call(
        output_kernel,
        out_shape=(shape, shape),
        in_specs=[near, near],
        out_specs=(anywhere, anywhere),
        scratch_shapes=[pltpu.SemaphoreType.DMA((2,))],
    )(
        pltpu.with_memory_space_constraint(result, pltpu.VMEM),
        pltpu.with_memory_space_constraint(speed, pltpu.VMEM),
    )


def solution(mesh):
    return jax.shard_map(
        body,
        mesh=mesh,
        in_specs=(P("grp", None, "gz", "gy", None), P("grp", None)),
        out_specs=(P("grp", None, "gz", "gy", None), P("grp", None, "gz", "gy", None)),
        check_vma=False,
    )
```

```python
import functools
import math

import jax
import jax.numpy as jnp
import numpy as np
from jax import lax
from jax.experimental import pallas as pl
from jax.experimental.pallas import tpu as pltpu
from jax.sharding import PartitionSpec as P

TIME_STEP = 0.4
MESH = pl.DeviceIdType.MESH
N = 256
HALF = 128
GY = 4
GZ = 32
PEERS = GY * GZ
LZ = 8
LY = 64


def split(values):
    high = values.astype(jnp.bfloat16)
    low = (values - high.astype(jnp.float32)).astype(jnp.bfloat16)
    return high, low


def table_pair(table):
    table = np.asarray(table, np.float32)
    high = table.astype(jnp.bfloat16)
    low = (table - high.astype(np.float32)).astype(jnp.bfloat16)
    return np.stack([high, low])


def make_tables():
    index = np.arange(N)
    angle = (index[:, None] * index[None, :] % N) * (2.0 * math.pi / N)
    cosine, sine = np.cos(angle), np.sin(angle)
    alternate = 1.0 - 2.0 * (index % 2)
    sine_in = -sine[:HALF].copy()
    sine_in[0] = alternate
    x_in = np.concatenate([cosine[:HALF], sine_in], 0)
    x_out = 2.0 * x_in / N
    x_out[0] *= 0.5
    x_out[HALF] *= 0.5
    cos_y = cosine.reshape(GY, 1, LY, N)
    sin_y = sine.reshape(GY, 1, LY, N)
    to_real = np.concatenate([cos_y, sin_y], 1).reshape(2 * N, N)
    to_imag = np.concatenate([-sin_y, cos_y], 1).reshape(2 * N, N)
    y_in = np.concatenate([to_real, to_imag], 1)
    z_all = np.stack([cosine, sine])
    edges = x_out[:, [N - 3, N - 2, N - 1, 0]].T.reshape(4, 2, HALF, 1)
    x_edge = np.broadcast_to(edges, (4, 2, HALF, LY)).transpose(0, 2, 1, 3).reshape(4, HALF, 128)
    pairs = [table_pair(t) for t in (x_in, y_in, z_all, x_out)]
    return pairs + [np.asarray(x_edge, np.float32)]


def dot3(a, b, dims=((1,), (0,))):
    def one(left, right):
        return lax.dot_general(left, right, (dims, ((), ())), preferred_element_type=jnp.float32)

    return one(a[0], b[0]) + (one(a[0], b[1]) + one(a[1], b[0]))


def each_peer(gy, gz, visit):
    for q in range(1, GY):
        visit(lax.rem(gy + q, GY), gz)

    def step(k, carry):
        other_z = lax.rem(gz + k, GZ)
        for q in range(GY):
            visit(lax.rem(gy + q, GY), other_z)
        return carry

    lax.fori_loop(1, GZ, step, 0)


def wait_bytes(ref, sem):
    pltpu.make_async_copy(ref, ref, sem).wait()


def waves(shape, axis):
    index = lax.broadcasted_iota(jnp.int32, shape, axis)
    signed = jnp.where(index < N // 2, index, index - N)
    full = signed.astype(jnp.float32) * (2.0 * math.pi / N)
    return full, jnp.where(index == N // 2, 0.0, full)


def kernel_weight(offset):
    mag = jnp.abs(offset)
    square = mag * mag
    inner = 1.0 + square * (1.5 * mag - 2.5)
    rest = 2.0 - mag
    outer = 0.5 * rest * rest * (1.0 - mag)
    return jnp.where(mag < 1.0, inner, jnp.where(mag < 2.0, outer, 0.0 * mag))


def moved_by(values, steps, axis):
    return pltpu.roll(values, steps % values.shape[axis], axis)


def step_kernel(
    field_in, wind, x_in_h, y_in_h, z_all_h, x_out_h, x_edge_h, result, speed,
    field, x_in, y_in, z_all, x_out, x_edge, send, recv, stream, send2, recv2, scale, weight_x, weight_y, weight_z,
    moved, row_out, row_in, edge_out, edge_in, field_edge_out, field_edge_in,
    lateral_out, lateral_in, layer_out, layer_in,
    near_out, near_in, corner_in, corner,
    ssem, rsem, ssem2, rsem2, plane_s, plane_r, row_s, row_r, edge_s, edge_r,
    lateral_s, lateral_r, layer_s, layer_r, load_s,
    near_s, near_r, corner_s, corner_r,
):
    grp = lax.axis_index("grp")
    gy = lax.axis_index("gy")
    gz = lax.axis_index("gz")
    me = gy * GZ + gz
    is_wake = grp == 1
    next_y, last_y = lax.rem(gy + 1, GY), lax.rem(gy + GY - 1, GY)
    next_z, last_z = lax.rem(gz + 1, GZ), lax.rem(gz + GZ - 1, GZ)
    barrier = pltpu.get_barrier_semaphore()

    def remote(source, target, sems, device):
        pltpu.make_async_remote_copy(
            source, target, sems[0], sems[1], device_id=device, device_id_type=MESH
        ).start()

    def greet(other_y, other_z):
        pl.semaphore_signal(
            barrier, inc=1, device_id={"gy": other_y, "gz": other_z}, device_id_type=MESH
        )

    def load(source, target, index):
        pltpu.make_async_copy(source, target, load_s.at[index]).start()

    load(x_in_h, x_in, 3)
    for c in (1, 2, 0):
        load(field_in.at[0, c], field.at[0, c], c)
    load(y_in_h, y_in, 4)
    load(z_all_h, z_all, 5)
    load(x_out_h, x_out, 6)
    load(x_edge_h, x_edge, 7)
    each_peer(gy, gz, greet)
    around = ({}, {"gy": next_y}, {"gy": last_y}, {"gz": next_z}, {"gz": last_z})
    for place in around:
        pl.semaphore_signal(
            barrier, inc=1, device_id={"grp": 1 - grp, **place}, device_id_type=MESH
        )

    lane = lax.broadcasted_iota(jnp.int32, (HALF, 128), 1)
    first_half = lane < LY
    wait_bytes(x_in, load_s.at[3])
    for c in (1, 2, 0):
        wait_bytes(field.at[0, c], load_s.at[c])
        for b in range(2):
            rows = field[0, c, 4 * b : 4 * b + 4].reshape(4 * LY, N)
            lines = dot3((x_in[0], x_in[1]), split(rows), ((1,), (1,)))
            for t in range(2):
                real = lines[:HALF, 128 * t : 128 * t + 128]
                imag = lines[HALF:, 128 * t : 128 * t + 128]
                even = jnp.where(first_half, real, pltpu.roll(imag, LY, 1))
                odd = jnp.where(first_half, pltpu.roll(real, LY, 1), imag)
                z = 4 * b + 2 * t
                send[c, pl.ds(z, HALF, stride=LZ), :] = even
                send[c, pl.ds(z + 1, HALF, stride=LZ), :] = odd
    mine = pl.ds(pl.multiple_of(me * LZ, LZ), LZ)
    mine_z = pl.ds(pl.multiple_of(gz * LZ, LZ), LZ)

    @pl.when(grp == 0)
    def _():
        for c in range(3):
            for z in range(0, LZ, 2):
                turned = field[0, c, z : z + 2, :, 128:].reshape(2 * LY, 128).T[120:]
                other = pltpu.roll(turned, LY, 1)
                for q in range(2):
                    field_edge_out[c, q, z : z + 1, :] = turned[6 + q : 7 + q]
                    field_edge_out[c, q, z + 1 : z + 2, :] = other[6 + q : 7 + q]

    pl.semaphore_wait(barrier, PEERS - 1 + len(around))

    for c in (1, 2, 0):
        def out(other_y, other_z, c=c):
            other = other_y * GZ + other_z
            remote(
                send.at[c, pl.ds(pl.multiple_of(other * LZ, LZ), LZ)],
                recv.at[c, gy, mine_z],
                (ssem.at[c], rsem.at[c]),
                {"gy": other_y, "gz": other_z},
            )

        each_peer(gy, gz, out)
        recv[c, gy, mine_z, :] = send[c, mine, :]

    @pl.when(grp == 0)
    def _():
        remote(field_edge_out, field_edge_in, (load_s.at[8], load_s.at[9]), {"grp": 1})

    wave_z, curl_z = waves((N, N), 0)
    wave_y, curl_y = waves((N, N), 1)
    curl_x = me.astype(jnp.float32) * (2.0 * math.pi / N)
    squared = curl_x * curl_x + wave_y * wave_y + wave_z * wave_z
    positive = squared > 0
    scale[0] = jnp.where(positive, 1.0 / jnp.where(positive, squared, 1.0), 0.0)

    @pl.when(me == 0)
    def _():
        base = scale[0]
        top = 1.0 / (squared + math.pi * math.pi)
        scale[0] = 0.5 * (base + top)
        scale[1] = 0.5 * (base - top)

    wait_bytes(y_in, load_s.at[4])
    wait_bytes(z_all, load_s.at[5])
    wait_bytes(x_out, load_s.at[6])
    wait_bytes(x_edge, load_s.at[7])
    curl = (curl_x, curl_y, curl_z)
    table_y = (y_in[0], y_in[1])
    cosine = (z_all[0, 0], z_all[1, 0])
    sine = (z_all[0, 1], z_all[1, 1])

    def transform(plane):
        lines = split(dot3(split(plane), table_y))
        by_cos = dot3(cosine, lines)
        by_sin = dot3(sine, lines)
        real = by_cos[:, :N] + by_sin[:, N:]
        imag = by_cos[:, N:] - by_sin[:, :N]
        return real, imag

    def forward(c):
        wait_bytes(recv2.at[c, pl.ds(0, (PEERS - 1) * LZ)], rsem.at[c])
        plane = jnp.concatenate([recv[c, j] for j in range(GY)], 1)
        real, imag = transform(plane)
        stream[c, 0] = real * scale[0]
        stream[c, 1] = imag * scale[0]

        @pl.when(me == 0)
        def _():
            column = lax.broadcasted_iota(jnp.int32, (N, 2 * N), 1)
            plane = jnp.concatenate([recv[c, j] for j in range(GY)], 1)
            real, imag = transform(jnp.where(column % 128 < LY, plane, -plane))
            stream[c, 0] += real * scale[1]
            stream[c, 1] += imag * scale[1]

    def backward(d):
        a, b = (d + 1) % 3, (d + 2) % 3
        real = curl[b] * stream[a, 1] - curl[a] * stream[b, 1]
        imag = curl[a] * stream[b, 0] - curl[b] * stream[a, 0]
        lines = split(jnp.concatenate([real, imag], 1))
        by_cos = dot3(cosine, lines)
        by_sin = dot3(sine, lines)
        real = by_cos[:, :N] - by_sin[:, N:]
        imag = by_cos[:, N:] + by_sin[:, :N]
        lines = split(jnp.concatenate([real, imag], 1) * (1.0 / (N * N)))
        plane = dot3(lines, table_y, ((1,), (1,)))
        for j in range(GY):
            send2[d, j] = plane[:, 128 * j : 128 * j + 128]

    def send_back(d):
        def out(other_y, other_z):
            remote(
                send2.at[d, other_y, pl.ds(pl.multiple_of(other_z * LZ, LZ), LZ)],
                recv2.at[d, mine],
                (ssem2.at[d], rsem2.at[d]),
                {"gy": other_y, "gz": other_z},
            )

        each_peer(gy, gz, out)
        recv2[d, mine, :] = send2[d, gy, mine_z, :]

    forward(1)
    forward(2)
    backward(0)
    send_back(0)
    forward(0)
    backward(1)
    send_back(1)
    backward(2)

    row = lax.broadcasted_iota(jnp.int32, (LY, N), 0)
    column = lax.broadcasted_iota(jnp.int32, (LY, N), 1)
    tile = lax.broadcasted_iota(jnp.int32, (LY, 128), 1)
    short_row = lax.broadcasted_iota(jnp.int32, (8, N), 0)
    no_wrap_low = jnp.where(is_wake, 0, -N)
    no_wrap_high = jnp.where(is_wake, N, 2 * N)
    first_column = jnp.where(is_wake, 0, -1)
    small_lane = lax.broadcasted_iota(jnp.int32, (LZ, 128), 1)
    small_row = lax.broadcasted_iota(jnp.int32, (LZ, 128), 0)
    last_column = jnp.where(is_wake, N - 1, N)

    def velocity_of(d):
        wait_bytes(recv.at[0, :, pl.ds(0, (PEERS - 1) * LZ // GY)], rsem2.at[d])
        drift = wind[0, d]

        for b in range(2):
            parts = []
            for z in range(4 * b, 4 * b + 4):
                turned = recv2[d, pl.ds(z, HALF, stride=LZ), :].T
                parts.append(jnp.concatenate([turned[:LY], turned[LY:]], 1))
            lines = split(jnp.concatenate(parts, 0))
            out = dot3(lines, (x_out[0], x_out[1])) + drift
            for z in range(4 * b, 4 * b + 4):
                plane = out[LY * (z - 4 * b) : LY * (z - 4 * b) + LY]
                speed[d, z + 1] = plane
                row_out[0, d * LZ + z : d * LZ + z + 1, :] = plane[LY - 1 :]
                row_out[1, d * LZ + z : d * LZ + z + 1, :] = plane[:1]
                if d == 2 and z in (0, 1, LZ - 2, LZ - 1):
                    side, start = (1, 4 * z) if z < 2 else (0, 4 * (z - LZ + 2))
                    near_out[side, start : start + 2, :] = plane[:2]
                    near_out[side, start + 2 : start + 4, :] = plane[LY - 2 :]
            if b == 0:
                remote(
                    speed.at[d, 1],
                    speed.at[d, LZ + 1],
                    (plane_s.at[d], plane_r.at[d]),
                    {"gz": last_z},
                )
        rows = pl.ds(d * LZ, LZ)
        remote(speed.at[d, LZ], speed.at[d, 0], (plane_s.at[d], plane_r.at[d]), {"gz": next_z})
        remote(row_out.at[0, rows], row_in.at[0, rows], (row_s.at[d], row_r.at[d]), {"gy": next_y})
        remote(row_out.at[1, rows], row_in.at[1, rows], (row_s.at[d], row_r.at[d]), {"gy": last_y})
        if d == 2:
            for side, other in ((0, next_z), (1, last_z)):
                remote(near_out.at[side], near_in.at[side], (near_s, near_r), {"gz": other})

        @pl.when(grp == 0)
        def _():
            def add(i, totals):
                for k in range(8):
                    line = 8 * i + k
                    lines = recv2[d, pl.ds(pl.multiple_of(line * LZ, LZ), LZ), :]
                    totals = [t + lines * x_edge[q, pl.ds(line, 1), :] for q, t in enumerate(totals)]
                return tuple(totals)

            zero = jnp.zeros((LZ, 128), jnp.float32)
            totals = lax.fori_loop(0, HALF // 8, add, (zero,) * 4)
            for q in range(4):
                edge_out[d, q] = totals[q] + pltpu.roll(totals[q], LY, 1) + drift
            sems = (edge_s.at[d], edge_r.at[d])
            remote(edge_out.at[d], edge_in.at[d, 0], sems, {"grp": 1})
            for slot in range(1, 5):
                remote(
                    edge_out.at[d, pl.ds(1, 2)],
                    edge_in.at[d, slot, pl.ds(1, 2)],
                    sems,
                    {"grp": 1, **around[slot]},
                )

    def weights(target, d):
        def at(z, carry):
            shift = TIME_STEP * speed[d, z + 1]
            for offset in range(-2, 3):
                value = kernel_weight(offset - shift)
                if d == 0 and offset > 0:
                    value = jnp.where(column >= no_wrap_high - offset, 0.0, value)
                if d == 0 and offset < 0:
                    value = jnp.where(column < no_wrap_low - offset, 0.0, value)
                target[offset + 2, z] = value
            return carry

        lax.fori_loop(0, LZ, at, 0)

    def stretch(d):
        wait_bytes(speed.at[d, pl.ds(0, 2)], plane_r.at[d])
        wait_bytes(row_in.at[0, pl.ds(0, 2 * LZ)], row_r.at[d])

        def at(z, carry):
            here = speed[d, z + 1]
            grad_z = speed[d, z + 2] - speed[d, z]
            low = row_in[0, pl.ds(d * LZ + z, 1), :]
            high = row_in[1, pl.ds(d * LZ + z, 1), :]
            up = jnp.where(row == LY - 1, high, moved_by(here, -1, 0))
            down = jnp.where(row == 0, low, moved_by(here, 1, 0))
            left = moved_by(here, 1, 1)
            left = jnp.concatenate(
                [jnp.where(tile == first_column, 0.0, left[:, :128]), left[:, 128:]], 1
            )
            right = jnp.where(column == last_column, here, moved_by(here, -1, 1))
            strength = field[0, d, z] + (0.5 * TIME_STEP) * (
                field[0, 0, z] * (right - left)
                + field[0, 1, z] * (up - down)
                + field[0, 2, z] * grad_z
            )
            one = moved_by(strength * weight_x[3, z], 1, 1)
            two = moved_by(strength * weight_x[4, z], 2, 1)
            total = strength * weight_x[2, z] + one + two
            total = total + moved_by(strength * weight_x[1, z], -1, 1)
            moved[d, z] = total + moved_by(strength * weight_x[0, z], -2, 1)
            return carry

        lax.fori_loop(0, LZ, at, 0)

    def lateral_send(d):
        @pl.when(is_wake)
        def _():
            wait_bytes(edge_in.at[d, pl.ds(0, 3)], edge_r.at[d])
            if d == 0:
                wait_bytes(field_edge_in, load_s.at[9])

            def particle(q, grad_x):
                here = edge_in[d, 0, q]
                low_y, high_y = edge_in[d, 1, q], edge_in[d, 2, q]
                low_z, high_z = edge_in[d, 3, q], edge_in[d, 4, q]
                up = jnp.where(small_lane == LY - 1, moved_by(high_y, -1, 1), moved_by(here, -1, 1))
                down = jnp.where(small_lane == 0, moved_by(low_y, 1, 1), moved_by(here, 1, 1))
                above = jnp.where(small_row == LZ - 1, moved_by(high_z, -1, 0), moved_by(here, -1, 0))
                below = jnp.where(small_row == 0, moved_by(low_z, 1, 0), moved_by(here, 1, 0))
                return field_edge_in[d, q - 1] + (0.5 * TIME_STEP) * (
                    field_edge_in[0, q - 1] * grad_x
                    + field_edge_in[1, q - 1] * (up - down)
                    + field_edge_in[2, q - 1] * (above - below)
                )

            strength_one = particle(2, edge_in[d, 0, 3] - edge_in[d, 0, 1])
            strength_two = particle(1, edge_in[d, 0, 2] - edge_in[d, 0, 0])
            shift_one = TIME_STEP * edge_in[0, 0, 2]
            shift_two = TIME_STEP * edge_in[0, 0, 1]
            first = strength_one * kernel_weight(1 - shift_one) + strength_two * kernel_weight(
                2 - shift_two
            )
            second = strength_one * kernel_weight(2 - shift_one)
            empty = jnp.zeros((128 - 3 * LZ, 128), jnp.float32)
            turned = jnp.concatenate([edge_in[d, 0, 2], first, second, empty], 0).T[:LY]

            def add(z, carry):
                inflow = jnp.where(tile == 0, pltpu.roll(turned, lax.rem(128 - z, 128), 1), 0.0)
                missing = (-0.5 * TIME_STEP) * field[0, 0, z, :, :128] * inflow
                total = missing * weight_x[2, z, :, :128]
                total = total + pltpu.roll(missing * weight_x[3, z, :, :128], 1, 1)
                total = total + pltpu.roll(missing * weight_x[4, z, :, :128], 2, 1)
                total = total + jnp.where(tile == 0, pltpu.roll(turned, 120 - z, 1), 0.0)
                total = total + jnp.where(tile == 1, pltpu.roll(turned, 113 - z, 1), 0.0)
                moved[d, z, :, :128] += total
                return carry

            lax.fori_loop(0, LZ, add, 0)

        def at(z, carry):
            here = moved[d, z]
            one = moved_by(here * weight_y[3, z], 1, 0)
            two = moved_by(here * weight_y[4, z], 2, 0)
            back_one = moved_by(here * weight_y[1, z], -1, 0)
            back_two = moved_by(here * weight_y[0, z], -2, 0)
            total = here * weight_y[2, z]
            total = total + jnp.where(row < 1, 0.0, one) + jnp.where(row < 2, 0.0, two)
            total = total + jnp.where(row >= LY - 1, 0.0, back_one)
            moved[d, z] = total + jnp.where(row >= LY - 2, 0.0, back_two)
            at_z = pl.ds(d * LZ + z, 1)
            lateral_out[0, 0, at_z, :] = one[0:1] + two[0:1]
            lateral_out[0, 1, at_z, :] = two[1:2]
            lateral_out[1, 0, at_z, :] = back_two[LY - 2 : LY - 1]
            lateral_out[1, 1, at_z, :] = back_one[LY - 1 :] + back_two[LY - 1 :]
            return carry

        lax.fori_loop(0, LZ, at, 0)
        rows = pl.ds(d * LZ, LZ)
        for side, other in ((0, next_y), (1, last_y)):
            for step in range(2):
                remote(
                    lateral_out.at[side, step, rows],
                    lateral_in.at[side, step, rows],
                    (lateral_s.at[d], lateral_r.at[d]),
                    {"gy": other},
                )
        if d == 2:
            for side, other in ((0, next_y), (1, last_y)):
                for level, far in ((0, next_z), (1, last_z)):
                    remote(
                        lateral_out.at[side, :, rows],
                        corner_in.at[side, level],
                        (corner_s, corner_r),
                        {"gy": other, "gz": far},
                    )

    def lateral_rows(d, z):
        at_z = pl.ds(d * LZ + z, 1)
        first, second = lateral_in[0, 0, at_z, :], lateral_in[0, 1, at_z, :]
        third, fourth = lateral_in[1, 0, at_z, :], lateral_in[1, 1, at_z, :]
        low = jnp.where(short_row == 0, first, jnp.where(short_row == 1, second, 0.0))
        high = jnp.where(short_row == 6, third, jnp.where(short_row == 7, fourth, 0.0))
        return low, high

    def lateral_add(d):
        wait_bytes(row_in.at[:, pl.ds(0, 2 * LZ)], lateral_r.at[d])

        def add(z, carry):
            low, high = lateral_rows(d, z)
            moved[d, z, :8] += low
            moved[d, z, LY - 8 :] += high
            return carry

        lax.fori_loop(0, LZ, add, 0)

    def layers_send(d):
        end = LZ - 1
        layer_out[0, d, 0] = moved[d, end] * weight_z[3, end] + moved[d, end - 1] * weight_z[4, end - 1]
        layer_out[0, d, 1] = moved[d, end] * weight_z[4, end]
        layer_out[1, d, 0] = moved[d, 0] * weight_z[0, 0]
        layer_out[1, d, 1] = moved[d, 0] * weight_z[1, 0] + moved[d, 1] * weight_z[0, 1]
        for side, other in ((0, next_z), (1, last_z)):
            remote(
                layer_out.at[side, d],
                layer_in.at[side, d],
                (layer_s.at[d], layer_r.at[d]),
                {"gz": other},
            )
        for z in range(LZ):
            total = moved[d, z] * weight_z[2, z]
            for offset in (-2, -1, 1, 2):
                if 0 <= z - offset < LZ:
                    total = total + moved[d, z - offset] * weight_z[offset + 2, z - offset]
            result[d, z] = total

    def late_rows(d):
        wait_bytes(row_in.at[:, pl.ds(0, 2 * LZ)], lateral_r.at[d])
        for z in range(LZ):
            for start, part in zip((0, LY - 8), lateral_rows(d, z)):
                rows = slice(start, start + 8)
                for offset in range(-2, 3):
                    if 0 <= z + offset < LZ:
                        result[d, z + offset, rows] += part * weight_z[offset + 2, z, rows]
        wait_bytes(near_in, near_r)
        wait_bytes(corner_in, corner_r)
        for level in range(2):
            for plane in range(2):
                z = plane if level else LZ - 2 + plane
                for side in range(2):
                    for step in range(2):
                        at_row = 4 * plane + 2 * side + step
                        corner[level, at_row : at_row + 1, :] = corner_in[side, level, step, z : z + 1]
        shift = TIME_STEP * near_in[0]
        one = corner[0] * kernel_weight(1 - shift)
        two = corner[0] * kernel_weight(2 - shift)
        parts = [(0, one[4:] + two[:4]), (1, two[4:])]
        shift = TIME_STEP * near_in[1]
        one = corner[1] * kernel_weight(-1 - shift)
        two = corner[1] * kernel_weight(-2 - shift)
        parts += [(LZ - 1, one[:4] + two[4:]), (LZ - 2, two[:4])]
        for z, part in parts:
            result[d, z, :2] += part[:2]
            result[d, z, LY - 2 :] += part[2:]

    def finish(d):
        wait_bytes(layer_in.at[:, d], layer_r.at[d])
        for side, start in ((0, 0), (1, LZ - 2)):
            for step in range(2):
                result[d, start + step] += layer_in[side, d, step]

    velocity_of(0)
    send_back(2)
    weights(weight_x, 0)
    stretch(0)
    velocity_of(1)
    weights(weight_y, 1)
    lateral_send(0)
    stretch(1)
    velocity_of(2)
    weights(weight_z, 2)
    lateral_add(0)
    layers_send(0)
    lateral_send(1)
    stretch(2)
    lateral_add(1)
    layers_send(1)
    lateral_send(2)
    layers_send(2)
    finish(0)
    finish(1)
    late_rows(2)
    finish(2)

    wait_bytes(near_out, near_s)
    wait_bytes(corner_in, corner_s)
    for c in range(3):
        wait_bytes(send.at[c, pl.ds(0, (PEERS - 1) * LZ)], ssem.at[c])
        wait_bytes(send.at[c, pl.ds(0, (PEERS - 1) * LZ)], ssem2.at[c])
        wait_bytes(speed.at[c, pl.ds(0, 2)], plane_s.at[c])
        wait_bytes(row_out.at[0, pl.ds(0, 2 * LZ)], row_s.at[c])
        wait_bytes(row_out.at[:, pl.ds(0, 2 * LZ)], lateral_s.at[c])
        wait_bytes(layer_out.at[:, c], layer_s.at[c])

        @pl.when(grp == 0)
        def _():
            wait_bytes(edge_in.at[c, pl.ds(0, 3)], edge_s.at[c])
            if c == 0:
                wait_bytes(field_edge_out, load_s.at[8])


def output_kernel(result, speed, result_out, velocity_out, sems):
    copies = [
        pltpu.make_async_copy(speed.at[:, pl.ds(1, LZ)], velocity_out.at[0], sems.at[0]),
        pltpu.make_async_copy(result, result_out.at[0], sems.at[1]),
    ]
    for copy in copies:
        copy.start()
    for copy in copies:
        copy.wait()


def body(vorticity, wind):
    tables = [jnp.asarray(t) for t in make_tables()]
    anywhere = pl.BlockSpec(memory_space=pl.ANY)
    near = pl.BlockSpec(memory_space=pltpu.VMEM)
    shape = jax.ShapeDtypeStruct(vorticity.shape, jnp.float32)
    block = (3, LZ, LY, N)
    buffers = [
        (3, PEERS * LZ, 128),
        (3, GY, N, 128),
        (3, 2, N, N),
        (3, GY, N, 128),
        (3, PEERS * LZ, 128),
        (2, N, N),
        (5, LZ, LY, N),
        (5, LZ, LY, N),
        (5, LZ, LY, N),
        block,
        (2, 3 * LZ, N),
        (2, 3 * LZ, N),
        (3, 4, LZ, 128),
        (3, 5, 4, LZ, 128),
        (3, 2, LZ, 128),
        (3, 2, LZ, 128),
        (2, 2, 3 * LZ, N),
        (2, 2, 3 * LZ, N),
        (2, 3, 2, LY, N),
        (2, 3, 2, LY, N),
        (2, 8, N),
        (2, 8, N),
        (2, 2, 2, LZ, N),
        (2, 8, N),
    ]
    result, speed = pl.pallas_call(
        step_kernel,
        out_shape=(pltpu.VMEM(block, jnp.float32), pltpu.VMEM((3, LZ + 2, LY, N), jnp.float32)),
        in_specs=[anywhere, pl.BlockSpec(memory_space=pltpu.SMEM)] + [anywhere] * 5,
        out_specs=(pl.BlockSpec(memory_space=pltpu.VMEM), pl.BlockSpec(memory_space=pltpu.VMEM)),
        scratch_shapes=[pltpu.VMEM(vorticity.shape, jnp.float32)]
        + [pltpu.VMEM(t.shape, t.dtype) for t in tables]
        + [pltpu.VMEM(b, jnp.float32) for b in buffers]
        + [pltpu.SemaphoreType.DMA((3,))] * 14
        + [pltpu.SemaphoreType.DMA((10,))]
        + [pltpu.SemaphoreType.DMA] * 4,
        compiler_params=pltpu.CompilerParams(collective_id=0, has_side_effects=True),
    )(vorticity, wind, *tables)
    return pl.pallas_call(
        output_kernel,
        out_shape=(shape, shape),
        in_specs=[near, near],
        out_specs=(anywhere, anywhere),
        scratch_shapes=[pltpu.SemaphoreType.DMA((2,))],
    )(
        pltpu.with_memory_space_constraint(result, pltpu.VMEM),
        pltpu.with_memory_space_constraint(speed, pltpu.VMEM),
    )


def solution(mesh):
    return jax.shard_map(
        body,
        mesh=mesh,
        in_specs=(P("grp", None, "gz", "gy", None), P("grp", None)),
        out_specs=(P("grp", None, "gz", "gy", None), P("grp", None, "gz", "gy", None)),
        check_vma=False,
    )
```

```python
import functools
import math

import jax
import jax.numpy as jnp
import numpy as np
from jax import lax
from jax.experimental import pallas as pl
from jax.experimental.pallas import tpu as pltpu
from jax.sharding import PartitionSpec as P

TIME_STEP = 0.4
MESH = pl.DeviceIdType.MESH
N = 256
HALF = 128
GY = 4
GZ = 32
PEERS = GY * GZ
LZ = 8
LY = 64


def split(values):
    high = values.astype(jnp.bfloat16)
    low = (values - high.astype(jnp.float32)).astype(jnp.bfloat16)
    return high, low


def table_pair(table):
    table = np.asarray(table, np.float32)
    high = table.astype(jnp.bfloat16)
    low = (table - high.astype(np.float32)).astype(jnp.bfloat16)
    return np.stack([high, low])


def make_tables():
    index = np.arange(N)
    angle = (index[:, None] * index[None, :] % N) * (2.0 * math.pi / N)
    cosine, sine = np.cos(angle), np.sin(angle)
    alternate = 1.0 - 2.0 * (index % 2)
    sine_in = -sine[:HALF].copy()
    sine_in[0] = alternate
    x_in = np.concatenate([cosine[:HALF], sine_in], 0)
    x_out = 2.0 * x_in / N
    x_out[0] *= 0.5
    x_out[HALF] *= 0.5
    cos_y = cosine.reshape(GY, 1, LY, N)
    sin_y = sine.reshape(GY, 1, LY, N)
    to_real = np.concatenate([cos_y, sin_y], 1).reshape(2 * N, N)
    to_imag = np.concatenate([-sin_y, cos_y], 1).reshape(2 * N, N)
    y_in = np.concatenate([to_real, to_imag], 1)
    z_all = np.stack([cosine, sine])
    edges = x_out[:, [N - 3, N - 2, N - 1, 0]].T.reshape(4, 2, HALF, 1)
    x_edge = np.broadcast_to(edges, (4, 2, HALF, LY)).transpose(0, 2, 1, 3).reshape(4, HALF, 128)
    pairs = [table_pair(t) for t in (x_in, y_in, z_all, x_out)]
    return pairs + [np.asarray(x_edge, np.float32)]


def dot3(a, b, dims=((1,), (0,))):
    def one(left, right):
        return lax.dot_general(left, right, (dims, ((), ())), preferred_element_type=jnp.float32)

    return one(a[0], b[0]) + (one(a[0], b[1]) + one(a[1], b[0]))


def each_peer(gy, gz, visit):
    for q in range(1, GY):
        visit(lax.rem(gy + q, GY), gz)

    def step(k, carry):
        other_z = lax.rem(gz + k, GZ)
        for q in range(GY):
            visit(lax.rem(gy + q, GY), other_z)
        return carry

    lax.fori_loop(1, GZ, step, 0)


def wait_bytes(ref, sem):
    pltpu.make_async_copy(ref, ref, sem).wait()


def waves(shape, axis):
    index = lax.broadcasted_iota(jnp.int32, shape, axis)
    signed = jnp.where(index < N // 2, index, index - N)
    full = signed.astype(jnp.float32) * (2.0 * math.pi / N)
    return full, jnp.where(index == N // 2, 0.0, full)


def kernel_weight(offset):
    mag = jnp.abs(offset)
    inner = 1.0 + mag * mag * (1.5 * mag - 2.5)
    near = jnp.minimum(mag, 2.0)
    rest = 2.0 - near
    outer = rest * rest * (0.5 - 0.5 * near)
    return jnp.where(mag < 1.0, inner, outer)


def moved_by(values, steps, axis):
    return pltpu.roll(values, steps % values.shape[axis], axis)


def step_kernel(
    field_in, wind, x_in_h, y_in_h, z_all_h, x_out_h, x_edge_h, result, speed,
    field, x_in, y_in, z_all, x_out, x_edge, send, recv, stream, send2, recv2, scale, weight_x, weight_y, weight_z,
    moved, row_out, row_in, edge_out, edge_in, field_edge_out, field_edge_in,
    lateral_out, lateral_in, layer_out, layer_in,
    near_out, near_in, corner_in, corner,
    ssem, rsem, ssem2, rsem2, plane_s, plane_r, row_s, row_r, edge_s, edge_r,
    lateral_s, lateral_r, layer_s, layer_r, load_s,
    near_s, near_r, corner_s, corner_r,
):
    grp = lax.axis_index("grp")
    gy = lax.axis_index("gy")
    gz = lax.axis_index("gz")
    me = gy * GZ + gz
    is_wake = grp == 1
    next_y, last_y = lax.rem(gy + 1, GY), lax.rem(gy + GY - 1, GY)
    next_z, last_z = lax.rem(gz + 1, GZ), lax.rem(gz + GZ - 1, GZ)
    barrier = pltpu.get_barrier_semaphore()

    def remote(source, target, sems, device):
        pltpu.make_async_remote_copy(
            source, target, sems[0], sems[1], device_id=device, device_id_type=MESH
        ).start()

    def greet(other_y, other_z):
        pl.semaphore_signal(
            barrier, inc=1, device_id={"gy": other_y, "gz": other_z}, device_id_type=MESH
        )

    def load(source, target, index):
        pltpu.make_async_copy(source, target, load_s.at[index]).start()

    load(x_in_h, x_in, 3)
    for c in (1, 2, 0):
        load(field_in.at[0, c], field.at[0, c], c)
    load(y_in_h, y_in, 4)
    load(z_all_h, z_all, 5)
    load(x_out_h, x_out, 6)
    load(x_edge_h, x_edge, 7)
    each_peer(gy, gz, greet)
    around = ({}, {"gy": next_y}, {"gy": last_y}, {"gz": next_z}, {"gz": last_z})
    for place in around:
        pl.semaphore_signal(
            barrier, inc=1, device_id={"grp": 1 - grp, **place}, device_id_type=MESH
        )

    lane = lax.broadcasted_iota(jnp.int32, (HALF, 128), 1)
    first_half = lane < LY
    wait_bytes(x_in, load_s.at[3])
    for c in (1, 2, 0):
        wait_bytes(field.at[0, c], load_s.at[c])
        for b in range(2):
            rows = field[0, c, 4 * b : 4 * b + 4].reshape(4 * LY, N)
            lines = dot3((x_in[0], x_in[1]), split(rows), ((1,), (1,)))
            for t in range(2):
                real = lines[:HALF, 128 * t : 128 * t + 128]
                imag = lines[HALF:, 128 * t : 128 * t + 128]
                even = jnp.where(first_half, real, pltpu.roll(imag, LY, 1))
                odd = jnp.where(first_half, pltpu.roll(real, LY, 1), imag)
                z = 4 * b + 2 * t
                send[c, pl.ds(z, HALF, stride=LZ), :] = even
                send[c, pl.ds(z + 1, HALF, stride=LZ), :] = odd
    mine = pl.ds(pl.multiple_of(me * LZ, LZ), LZ)
    mine_z = pl.ds(pl.multiple_of(gz * LZ, LZ), LZ)

    @pl.when(grp == 0)
    def _():
        for c in range(3):
            for z in range(0, LZ, 2):
                turned = field[0, c, z : z + 2, :, 128:].reshape(2 * LY, 128).T[120:]
                other = pltpu.roll(turned, LY, 1)
                for q in range(2):
                    field_edge_out[c, q, z : z + 1, :] = turned[6 + q : 7 + q]
                    field_edge_out[c, q, z + 1 : z + 2, :] = other[6 + q : 7 + q]

    pl.semaphore_wait(barrier, PEERS - 1 + len(around))

    for c in (1, 2, 0):
        def out(other_y, other_z, c=c):
            other = other_y * GZ + other_z
            remote(
                send.at[c, pl.ds(pl.multiple_of(other * LZ, LZ), LZ)],
                recv.at[c, gy, mine_z],
                (ssem.at[c], rsem.at[c]),
                {"gy": other_y, "gz": other_z},
            )

        each_peer(gy, gz, out)
        recv[c, gy, mine_z, :] = send[c, mine, :]

    @pl.when(grp == 0)
    def _():
        remote(field_edge_out, field_edge_in, (load_s.at[8], load_s.at[9]), {"grp": 1})

    wave_z, curl_z = waves((N, N), 0)
    wave_y, curl_y = waves((N, N), 1)
    curl_x = me.astype(jnp.float32) * (2.0 * math.pi / N)
    squared = curl_x * curl_x + wave_y * wave_y + wave_z * wave_z
    positive = squared > 0
    scale[0] = jnp.where(positive, 1.0 / jnp.where(positive, squared, 1.0), 0.0)

    @pl.when(me == 0)
    def _():
        base = scale[0]
        top = 1.0 / (squared + math.pi * math.pi)
        scale[0] = 0.5 * (base + top)
        scale[1] = 0.5 * (base - top)

    wait_bytes(y_in, load_s.at[4])
    wait_bytes(z_all, load_s.at[5])
    wait_bytes(x_out, load_s.at[6])
    wait_bytes(x_edge, load_s.at[7])
    curl = (curl_x, curl_y, curl_z)
    table_y = (y_in[0], y_in[1])
    cosine = (z_all[0, 0], z_all[1, 0])
    sine = (z_all[0, 1], z_all[1, 1])

    def transform(plane):
        lines = split(dot3(split(plane), table_y))
        by_cos = dot3(cosine, lines)
        by_sin = dot3(sine, lines)
        real = by_cos[:, :N] + by_sin[:, N:]
        imag = by_cos[:, N:] - by_sin[:, :N]
        return real, imag

    def forward(c):
        wait_bytes(recv2.at[c, pl.ds(0, (PEERS - 1) * LZ)], rsem.at[c])
        plane = jnp.concatenate([recv[c, j] for j in range(GY)], 1)
        real, imag = transform(plane)
        stream[c, 0] = real * scale[0]
        stream[c, 1] = imag * scale[0]

        @pl.when(me == 0)
        def _():
            column = lax.broadcasted_iota(jnp.int32, (N, 2 * N), 1)
            plane = jnp.concatenate([recv[c, j] for j in range(GY)], 1)
            real, imag = transform(jnp.where(column % 128 < LY, plane, -plane))
            stream[c, 0] += real * scale[1]
            stream[c, 1] += imag * scale[1]

    def backward(d):
        a, b = (d + 1) % 3, (d + 2) % 3
        real = curl[b] * stream[a, 1] - curl[a] * stream[b, 1]
        imag = curl[a] * stream[b, 0] - curl[b] * stream[a, 0]
        lines = split(jnp.concatenate([real, imag], 1))
        by_cos = dot3(cosine, lines)
        by_sin = dot3(sine, lines)
        real = by_cos[:, :N] - by_sin[:, N:]
        imag = by_cos[:, N:] + by_sin[:, :N]
        lines = split(jnp.concatenate([real, imag], 1) * (1.0 / (N * N)))
        plane = dot3(lines, table_y, ((1,), (1,)))
        for j in range(GY):
            send2[d, j] = plane[:, 128 * j : 128 * j + 128]

    def send_back(d):
        def out(other_y, other_z):
            remote(
                send2.at[d, other_y, pl.ds(pl.multiple_of(other_z * LZ, LZ), LZ)],
                recv2.at[d, mine],
                (ssem2.at[d], rsem2.at[d]),
                {"gy": other_y, "gz": other_z},
            )

        each_peer(gy, gz, out)
        recv2[d, mine, :] = send2[d, gy, mine_z, :]

    forward(1)
    forward(2)
    backward(0)
    send_back(0)
    forward(0)
    backward(1)
    send_back(1)
    backward(2)

    row = lax.broadcasted_iota(jnp.int32, (LY, N), 0)
    column = lax.broadcasted_iota(jnp.int32, (LY, N), 1)
    tile = lax.broadcasted_iota(jnp.int32, (LY, 128), 1)
    short_row = lax.broadcasted_iota(jnp.int32, (8, N), 0)
    no_wrap_low = jnp.where(is_wake, 0, -N)
    no_wrap_high = jnp.where(is_wake, N, 2 * N)
    first_column = jnp.where(is_wake, 0, -1)
    small_lane = lax.broadcasted_iota(jnp.int32, (LZ, 128), 1)
    small_row = lax.broadcasted_iota(jnp.int32, (LZ, 128), 0)
    last_column = jnp.where(is_wake, N - 1, N)

    def velocity_of(d):
        wait_bytes(recv.at[0, :, pl.ds(0, (PEERS - 1) * LZ // GY)], rsem2.at[d])
        drift = wind[0, d]

        for b in range(2):
            parts = []
            for z in range(4 * b, 4 * b + 4):
                turned = recv2[d, pl.ds(z, HALF, stride=LZ), :].T
                parts.append(jnp.concatenate([turned[:LY], turned[LY:]], 1))
            lines = split(jnp.concatenate(parts, 0))
            out = dot3(lines, (x_out[0], x_out[1])) + drift
            for z in range(4 * b, 4 * b + 4):
                plane = out[LY * (z - 4 * b) : LY * (z - 4 * b) + LY]
                speed[d, z + 1] = plane
                row_out[0, d * LZ + z : d * LZ + z + 1, :] = plane[LY - 1 :]
                row_out[1, d * LZ + z : d * LZ + z + 1, :] = plane[:1]
                if d == 2 and z in (0, 1, LZ - 2, LZ - 1):
                    side, start = (1, 4 * z) if z < 2 else (0, 4 * (z - LZ + 2))
                    near_out[side, start : start + 2, :] = plane[:2]
                    near_out[side, start + 2 : start + 4, :] = plane[LY - 2 :]
            if b == 0:
                remote(
                    speed.at[d, 1],
                    speed.at[d, LZ + 1],
                    (plane_s.at[d], plane_r.at[d]),
                    {"gz": last_z},
                )
        rows = pl.ds(d * LZ, LZ)
        remote(speed.at[d, LZ], speed.at[d, 0], (plane_s.at[d], plane_r.at[d]), {"gz": next_z})
        remote(row_out.at[0, rows], row_in.at[0, rows], (row_s.at[d], row_r.at[d]), {"gy": next_y})
        remote(row_out.at[1, rows], row_in.at[1, rows], (row_s.at[d], row_r.at[d]), {"gy": last_y})
        if d == 2:
            for side, other in ((0, next_z), (1, last_z)):
                remote(near_out.at[side], near_in.at[side], (near_s, near_r), {"gz": other})

        @pl.when(grp == 0)
        def _():
            def add(i, totals):
                for k in range(8):
                    line = 8 * i + k
                    lines = recv2[d, pl.ds(pl.multiple_of(line * LZ, LZ), LZ), :]
                    totals = [t + lines * x_edge[q, pl.ds(line, 1), :] for q, t in enumerate(totals)]
                return tuple(totals)

            zero = jnp.zeros((LZ, 128), jnp.float32)
            totals = lax.fori_loop(0, HALF // 8, add, (zero,) * 4)
            for q in range(4):
                edge_out[d, q] = totals[q] + pltpu.roll(totals[q], LY, 1) + drift
            sems = (edge_s.at[d], edge_r.at[d])
            remote(edge_out.at[d], edge_in.at[d, 0], sems, {"grp": 1})
            for slot in range(1, 5):
                remote(
                    edge_out.at[d, pl.ds(1, 2)],
                    edge_in.at[d, slot, pl.ds(1, 2)],
                    sems,
                    {"grp": 1, **around[slot]},
                )

    def weights(target, d):
        def at(z, carry):
            shift = TIME_STEP * speed[d, z + 1]
            for offset in range(-2, 3):
                value = kernel_weight(offset - shift)
                if d == 0 and offset > 0:
                    value = jnp.where(column >= no_wrap_high - offset, 0.0, value)
                if d == 0 and offset < 0:
                    value = jnp.where(column < no_wrap_low - offset, 0.0, value)
                target[offset + 2, z] = value
            return carry

        lax.fori_loop(0, LZ, at, 0)

    def stretch(d):
        wait_bytes(speed.at[d, pl.ds(0, 2)], plane_r.at[d])
        wait_bytes(row_in.at[0, pl.ds(0, 2 * LZ)], row_r.at[d])

        def at(z, carry):
            here = speed[d, z + 1]
            grad_z = speed[d, z + 2] - speed[d, z]
            low = row_in[0, pl.ds(d * LZ + z, 1), :]
            high = row_in[1, pl.ds(d * LZ + z, 1), :]
            up = jnp.where(row == LY - 1, high, moved_by(here, -1, 0))
            down = jnp.where(row == 0, low, moved_by(here, 1, 0))
            left = moved_by(here, 1, 1)
            left = jnp.concatenate(
                [jnp.where(tile == first_column, 0.0, left[:, :128]), left[:, 128:]], 1
            )
            right = jnp.where(column == last_column, here, moved_by(here, -1, 1))
            strength = field[0, d, z] + (0.5 * TIME_STEP) * (
                field[0, 0, z] * (right - left)
                + field[0, 1, z] * (up - down)
                + field[0, 2, z] * grad_z
            )
            one = moved_by(strength * weight_x[3, z], 1, 1)
            two = moved_by(strength * weight_x[4, z], 2, 1)
            total = strength * weight_x[2, z] + one + two
            total = total + moved_by(strength * weight_x[1, z], -1, 1)
            moved[d, z] = total + moved_by(strength * weight_x[0, z], -2, 1)
            return carry

        lax.fori_loop(0, LZ, at, 0)

    def lateral_send(d):
        @pl.when(is_wake)
        def _():
            wait_bytes(edge_in.at[d, pl.ds(0, 3)], edge_r.at[d])
            if d == 0:
                wait_bytes(field_edge_in, load_s.at[9])

            def particle(q, grad_x):
                here = edge_in[d, 0, q]
                low_y, high_y = edge_in[d, 1, q], edge_in[d, 2, q]
                low_z, high_z = edge_in[d, 3, q], edge_in[d, 4, q]
                up = jnp.where(small_lane == LY - 1, moved_by(high_y, -1, 1), moved_by(here, -1, 1))
                down = jnp.where(small_lane == 0, moved_by(low_y, 1, 1), moved_by(here, 1, 1))
                above = jnp.where(small_row == LZ - 1, moved_by(high_z, -1, 0), moved_by(here, -1, 0))
                below = jnp.where(small_row == 0, moved_by(low_z, 1, 0), moved_by(here, 1, 0))
                return field_edge_in[d, q - 1] + (0.5 * TIME_STEP) * (
                    field_edge_in[0, q - 1] * grad_x
                    + field_edge_in[1, q - 1] * (up - down)
                    + field_edge_in[2, q - 1] * (above - below)
                )

            strength_one = particle(2, edge_in[d, 0, 3] - edge_in[d, 0, 1])
            strength_two = particle(1, edge_in[d, 0, 2] - edge_in[d, 0, 0])
            shift_one = TIME_STEP * edge_in[0, 0, 2]
            shift_two = TIME_STEP * edge_in[0, 0, 1]
            first = strength_one * kernel_weight(1 - shift_one) + strength_two * kernel_weight(
                2 - shift_two
            )
            second = strength_one * kernel_weight(2 - shift_one)
            empty = jnp.zeros((128 - 3 * LZ, 128), jnp.float32)
            turned = jnp.concatenate([edge_in[d, 0, 2], first, second, empty], 0).T[:LY]

            def add(z, carry):
                inflow = jnp.where(tile == 0, pltpu.roll(turned, lax.rem(128 - z, 128), 1), 0.0)
                missing = (-0.5 * TIME_STEP) * field[0, 0, z, :, :128] * inflow
                total = missing * weight_x[2, z, :, :128]
                total = total + pltpu.roll(missing * weight_x[3, z, :, :128], 1, 1)
                total = total + pltpu.roll(missing * weight_x[4, z, :, :128], 2, 1)
                total = total + jnp.where(tile == 0, pltpu.roll(turned, 120 - z, 1), 0.0)
                total = total + jnp.where(tile == 1, pltpu.roll(turned, 113 - z, 1), 0.0)
                moved[d, z, :, :128] += total
                return carry

            lax.fori_loop(0, LZ, add, 0)

        def at(z, carry):
            here = moved[d, z]
            one = moved_by(here * weight_y[3, z], 1, 0)
            two = moved_by(here * weight_y[4, z], 2, 0)
            back_one = moved_by(here * weight_y[1, z], -1, 0)
            back_two = moved_by(here * weight_y[0, z], -2, 0)
            total = here * weight_y[2, z]
            total = total + jnp.where(row < 1, 0.0, one) + jnp.where(row < 2, 0.0, two)
            total = total + jnp.where(row >= LY - 1, 0.0, back_one)
            moved[d, z] = total + jnp.where(row >= LY - 2, 0.0, back_two)
            at_z = pl.ds(d * LZ + z, 1)
            lateral_out[0, 0, at_z, :] = one[0:1] + two[0:1]
            lateral_out[0, 1, at_z, :] = two[1:2]
            lateral_out[1, 0, at_z, :] = back_two[LY - 2 : LY - 1]
            lateral_out[1, 1, at_z, :] = back_one[LY - 1 :] + back_two[LY - 1 :]
            return carry

        lax.fori_loop(0, LZ, at, 0)
        rows = pl.ds(d * LZ, LZ)
        for side, other in ((0, next_y), (1, last_y)):
            for step in range(2):
                remote(
                    lateral_out.at[side, step, rows],
                    lateral_in.at[side, step, rows],
                    (lateral_s.at[d], lateral_r.at[d]),
                    {"gy": other},
                )
        if d == 2:
            for side, other in ((0, next_y), (1, last_y)):
                for level, far in ((0, next_z), (1, last_z)):
                    remote(
                        lateral_out.at[side, :, rows],
                        corner_in.at[side, level],
                        (corner_s, corner_r),
                        {"gy": other, "gz": far},
                    )

    def lateral_rows(d, z):
        at_z = pl.ds(d * LZ + z, 1)
        first, second = lateral_in[0, 0, at_z, :], lateral_in[0, 1, at_z, :]
        third, fourth = lateral_in[1, 0, at_z, :], lateral_in[1, 1, at_z, :]
        low = jnp.where(short_row == 0, first, jnp.where(short_row == 1, second, 0.0))
        high = jnp.where(short_row == 6, third, jnp.where(short_row == 7, fourth, 0.0))
        return low, high

    def lateral_add(d):
        wait_bytes(row_in.at[:, pl.ds(0, 2 * LZ)], lateral_r.at[d])

        def add(z, carry):
            low, high = lateral_rows(d, z)
            moved[d, z, :8] += low
            moved[d, z, LY - 8 :] += high
            return carry

        lax.fori_loop(0, LZ, add, 0)

    def layers_send(d):
        end = LZ - 1
        layer_out[0, d, 0] = moved[d, end] * weight_z[3, end] + moved[d, end - 1] * weight_z[4, end - 1]
        layer_out[0, d, 1] = moved[d, end] * weight_z[4, end]
        layer_out[1, d, 0] = moved[d, 0] * weight_z[0, 0]
        layer_out[1, d, 1] = moved[d, 0] * weight_z[1, 0] + moved[d, 1] * weight_z[0, 1]
        for side, other in ((0, next_z), (1, last_z)):
            remote(
                layer_out.at[side, d],
                layer_in.at[side, d],
                (layer_s.at[d], layer_r.at[d]),
                {"gz": other},
            )
    def layers_within(d):
        for z in range(LZ):
            total = moved[d, z] * weight_z[2, z]
            for offset in (-2, -1, 1, 2):
                if 0 <= z - offset < LZ:
                    total = total + moved[d, z - offset] * weight_z[offset + 2, z - offset]
            result[d, z] = total

    def late_rows(d):
        wait_bytes(row_in.at[:, pl.ds(0, 2 * LZ)], lateral_r.at[d])
        for z in range(LZ):
            for start, part in zip((0, LY - 8), lateral_rows(d, z)):
                rows = slice(start, start + 8)
                for offset in range(-2, 3):
                    if 0 <= z + offset < LZ:
                        result[d, z + offset, rows] += part * weight_z[offset + 2, z, rows]
        wait_bytes(near_in, near_r)
        wait_bytes(corner_in, corner_r)
        for level in range(2):
            for plane in range(2):
                z = plane if level else LZ - 2 + plane
                for side in range(2):
                    for step in range(2):
                        at_row = 4 * plane + 2 * side + step
                        corner[level, at_row : at_row + 1, :] = corner_in[side, level, step, z : z + 1]
        shift = TIME_STEP * near_in[0]
        one = corner[0] * kernel_weight(1 - shift)
        two = corner[0] * kernel_weight(2 - shift)
        parts = [(0, one[4:] + two[:4]), (1, two[4:])]
        shift = TIME_STEP * near_in[1]
        one = corner[1] * kernel_weight(-1 - shift)
        two = corner[1] * kernel_weight(-2 - shift)
        parts += [(LZ - 1, one[:4] + two[4:]), (LZ - 2, two[:4])]
        for z, part in parts:
            result[d, z, :2] += part[:2]
            result[d, z, LY - 2 :] += part[2:]

    def finish(d):
        wait_bytes(layer_in.at[:, d], layer_r.at[d])
        for side, start in ((0, 0), (1, LZ - 2)):
            for step in range(2):
                result[d, start + step] += layer_in[side, d, step]

    velocity_of(0)
    send_back(2)
    weights(weight_x, 0)
    stretch(0)
    velocity_of(1)
    weights(weight_y, 1)
    lateral_send(0)
    stretch(1)
    velocity_of(2)
    weights(weight_z, 2)
    lateral_add(0)
    layers_send(0)
    lateral_send(1)
    stretch(2)
    lateral_add(1)
    layers_send(1)
    lateral_send(2)
    layers_send(2)
    layers_within(0)
    layers_within(1)
    layers_within(2)
    finish(0)
    finish(1)
    late_rows(2)
    finish(2)

    wait_bytes(near_out, near_s)
    wait_bytes(corner_in, corner_s)
    for c in range(3):
        wait_bytes(send.at[c, pl.ds(0, (PEERS - 1) * LZ)], ssem.at[c])
        wait_bytes(send.at[c, pl.ds(0, (PEERS - 1) * LZ)], ssem2.at[c])
        wait_bytes(speed.at[c, pl.ds(0, 2)], plane_s.at[c])
        wait_bytes(row_out.at[0, pl.ds(0, 2 * LZ)], row_s.at[c])
        wait_bytes(row_out.at[:, pl.ds(0, 2 * LZ)], lateral_s.at[c])
        wait_bytes(layer_out.at[:, c], layer_s.at[c])

        @pl.when(grp == 0)
        def _():
            wait_bytes(edge_in.at[c, pl.ds(0, 3)], edge_s.at[c])
            if c == 0:
                wait_bytes(field_edge_out, load_s.at[8])


def output_kernel(result, speed, result_out, velocity_out, sems):
    copies = [
        pltpu.make_async_copy(speed.at[:, pl.ds(1, LZ)], velocity_out.at[0], sems.at[0]),
        pltpu.make_async_copy(result, result_out.at[0], sems.at[1]),
    ]
    for copy in copies:
        copy.start()
    for copy in copies:
        copy.wait()


def body(vorticity, wind):
    tables = [jnp.asarray(t) for t in make_tables()]
    anywhere = pl.BlockSpec(memory_space=pl.ANY)
    near = pl.BlockSpec(memory_space=pltpu.VMEM)
    shape = jax.ShapeDtypeStruct(vorticity.shape, jnp.float32)
    block = (3, LZ, LY, N)
    buffers = [
        (3, PEERS * LZ, 128),
        (3, GY, N, 128),
        (3, 2, N, N),
        (3, GY, N, 128),
        (3, PEERS * LZ, 128),
        (2, N, N),
        (5, LZ, LY, N),
        (5, LZ, LY, N),
        (5, LZ, LY, N),
        block,
        (2, 3 * LZ, N),
        (2, 3 * LZ, N),
        (3, 4, LZ, 128),
        (3, 5, 4, LZ, 128),
        (3, 2, LZ, 128),
        (3, 2, LZ, 128),
        (2, 2, 3 * LZ, N),
        (2, 2, 3 * LZ, N),
        (2, 3, 2, LY, N),
        (2, 3, 2, LY, N),
        (2, 8, N),
        (2, 8, N),
        (2, 2, 2, LZ, N),
        (2, 8, N),
    ]
    result, speed = pl.pallas_call(
        step_kernel,
        out_shape=(pltpu.VMEM(block, jnp.float32), pltpu.VMEM((3, LZ + 2, LY, N), jnp.float32)),
        in_specs=[anywhere, pl.BlockSpec(memory_space=pltpu.SMEM)] + [anywhere] * 5,
        out_specs=(pl.BlockSpec(memory_space=pltpu.VMEM), pl.BlockSpec(memory_space=pltpu.VMEM)),
        scratch_shapes=[pltpu.VMEM(vorticity.shape, jnp.float32)]
        + [pltpu.VMEM(t.shape, t.dtype) for t in tables]
        + [pltpu.VMEM(b, jnp.float32) for b in buffers]
        + [pltpu.SemaphoreType.DMA((3,))] * 14
        + [pltpu.SemaphoreType.DMA((10,))]
        + [pltpu.SemaphoreType.DMA] * 4,
        compiler_params=pltpu.CompilerParams(collective_id=0, has_side_effects=True),
    )(vorticity, wind, *tables)
    return pl.pallas_call(
        output_kernel,
        out_shape=(shape, shape),
        in_specs=[near, near],
        out_specs=(anywhere, anywhere),
        scratch_shapes=[pltpu.SemaphoreType.DMA((2,))],
    )(
        pltpu.with_memory_space_constraint(result, pltpu.VMEM),
        pltpu.with_memory_space_constraint(speed, pltpu.VMEM),
    )


def solution(mesh):
    return jax.shard_map(
        body,
        mesh=mesh,
        in_specs=(P("grp", None, "gz", "gy", None), P("grp", None)),
        out_specs=(P("grp", None, "gz", "gy", None), P("grp", None, "gz", "gy", None)),
        check_vma=False,
    )
```

```python
import functools
import math

import jax
import jax.numpy as jnp
import numpy as np
from jax import lax
from jax.experimental import pallas as pl
from jax.experimental.pallas import tpu as pltpu
from jax.sharding import PartitionSpec as P

TIME_STEP = 0.4
MESH = pl.DeviceIdType.MESH
N = 256
HALF = 128
GY = 4
GZ = 32
PEERS = GY * GZ
LZ = 8
LY = 64


def split(values):
    high = values.astype(jnp.bfloat16)
    low = (values - high.astype(jnp.float32)).astype(jnp.bfloat16)
    return high, low


def table_pair(table):
    table = np.asarray(table, np.float32)
    high = table.astype(jnp.bfloat16)
    low = (table - high.astype(np.float32)).astype(jnp.bfloat16)
    return np.stack([high, low])


def make_tables():
    index = np.arange(N)
    angle = (index[:, None] * index[None, :] % N) * (2.0 * math.pi / N)
    cosine, sine = np.cos(angle), np.sin(angle)
    alternate = 1.0 - 2.0 * (index % 2)
    sine_in = -sine[:HALF].copy()
    sine_in[0] = alternate
    x_in = np.concatenate([cosine[:HALF], sine_in], 0)
    x_out = 2.0 * x_in / N
    x_out[0] *= 0.5
    x_out[HALF] *= 0.5
    cos_y = cosine.reshape(GY, 1, LY, N)
    sin_y = sine.reshape(GY, 1, LY, N)
    to_real = np.concatenate([cos_y, sin_y], 1).reshape(2 * N, N)
    to_imag = np.concatenate([-sin_y, cos_y], 1).reshape(2 * N, N)
    y_in = np.concatenate([to_real, to_imag], 1)
    z_all = np.stack([cosine, sine])
    edges = x_out[:, [N - 3, N - 2, N - 1, 0]].T.reshape(4, 2, HALF, 1)
    x_edge = np.broadcast_to(edges, (4, 2, HALF, LY)).transpose(0, 2, 1, 3).reshape(4, HALF, 128)
    pairs = [table_pair(t) for t in (x_in, y_in, z_all, x_out)]
    return pairs + [np.asarray(x_edge, np.float32)]


def dot3(a, b, dims=((1,), (0,))):
    def one(left, right):
        return lax.dot_general(left, right, (dims, ((), ())), preferred_element_type=jnp.float32)

    return one(a[0], b[0]) + (one(a[0], b[1]) + one(a[1], b[0]))


def each_peer(gy, gz, visit):
    for q in range(1, GY):
        visit(lax.rem(gy + q, GY), gz)

    def step(k, carry):
        other_z = lax.rem(gz + k, GZ)
        for q in range(GY):
            visit(lax.rem(gy + q, GY), other_z)
        return carry

    lax.fori_loop(1, GZ, step, 0)


def wait_bytes(ref, sem):
    pltpu.make_async_copy(ref, ref, sem).wait()


def waves(shape, axis):
    index = lax.broadcasted_iota(jnp.int32, shape, axis)
    signed = jnp.where(index < N // 2, index, index - N)
    full = signed.astype(jnp.float32) * (2.0 * math.pi / N)
    return full, jnp.where(index == N // 2, 0.0, full)


def kernel_weight(offset):
    mag = jnp.abs(offset)
    inner = 1.0 + mag * mag * (1.5 * mag - 2.5)
    near = jnp.minimum(mag, 2.0)
    rest = 2.0 - near
    outer = rest * rest * (0.5 - 0.5 * near)
    return jnp.where(mag < 1.0, inner, outer)


def moved_by(values, steps, axis):
    return pltpu.roll(values, steps % values.shape[axis], axis)


def step_kernel(
    field_in, wind, x_in_h, y_in_h, z_all_h, x_out_h, x_edge_h, result, speed,
    field, x_in, y_in, z_all, x_out, x_edge, send, recv, stream, send2, recv2, scale, weight_x, weight_y, weight_z,
    moved, row_out, row_in, edge_out, edge_in, field_edge_out, field_edge_in,
    lateral_out, lateral_in, layer_out, layer_in,
    near_out, near_in, corner_in, corner,
    ssem, rsem, ssem2, rsem2, plane_s, plane_r, row_s, row_r, edge_s, edge_r,
    lateral_s, lateral_r, layer_s, layer_r, load_s,
    near_s, near_r, corner_s, corner_r,
):
    grp = lax.axis_index("grp")
    gy = lax.axis_index("gy")
    gz = lax.axis_index("gz")
    me = gy * GZ + gz
    is_wake = grp == 1
    next_y, last_y = lax.rem(gy + 1, GY), lax.rem(gy + GY - 1, GY)
    next_z, last_z = lax.rem(gz + 1, GZ), lax.rem(gz + GZ - 1, GZ)
    barrier = pltpu.get_barrier_semaphore()

    def remote(source, target, sems, device):
        pltpu.make_async_remote_copy(
            source, target, sems[0], sems[1], device_id=device, device_id_type=MESH
        ).start()

    def greet(other_y, other_z):
        pl.semaphore_signal(
            barrier, inc=1, device_id={"gy": other_y, "gz": other_z}, device_id_type=MESH
        )

    def load(source, target, index):
        pltpu.make_async_copy(source, target, load_s.at[index]).start()

    load(x_in_h, x_in, 3)
    for c in (1, 2, 0):
        load(field_in.at[0, c], field.at[0, c], c)
    load(y_in_h, y_in, 4)
    load(z_all_h, z_all, 5)
    load(x_out_h, x_out, 6)
    load(x_edge_h, x_edge, 7)
    each_peer(gy, gz, greet)
    around = ({}, {"gy": next_y}, {"gy": last_y}, {"gz": next_z}, {"gz": last_z})
    for place in around:
        pl.semaphore_signal(
            barrier, inc=1, device_id={"grp": 1 - grp, **place}, device_id_type=MESH
        )

    lane = lax.broadcasted_iota(jnp.int32, (HALF, 128), 1)
    first_half = lane < LY
    wait_bytes(x_in, load_s.at[3])
    for c in (1, 2, 0):
        wait_bytes(field.at[0, c], load_s.at[c])
        for b in range(2):
            rows = field[0, c, 4 * b : 4 * b + 4].reshape(4 * LY, N)
            lines = dot3((x_in[0], x_in[1]), split(rows), ((1,), (1,)))
            for t in range(2):
                real = lines[:HALF, 128 * t : 128 * t + 128]
                imag = lines[HALF:, 128 * t : 128 * t + 128]
                even = jnp.where(first_half, real, pltpu.roll(imag, LY, 1))
                odd = jnp.where(first_half, pltpu.roll(real, LY, 1), imag)
                z = 4 * b + 2 * t
                send[c, pl.ds(z, HALF, stride=LZ), :] = even
                send[c, pl.ds(z + 1, HALF, stride=LZ), :] = odd
    mine = pl.ds(pl.multiple_of(me * LZ, LZ), LZ)
    mine_z = pl.ds(pl.multiple_of(gz * LZ, LZ), LZ)

    @pl.when(grp == 0)
    def _():
        for c in range(3):
            for z in range(0, LZ, 2):
                turned = field[0, c, z : z + 2, :, 128:].reshape(2 * LY, 128).T[120:]
                other = pltpu.roll(turned, LY, 1)
                for q in range(2):
                    field_edge_out[c, q, z : z + 1, :] = turned[6 + q : 7 + q]
                    field_edge_out[c, q, z + 1 : z + 2, :] = other[6 + q : 7 + q]

    pl.semaphore_wait(barrier, PEERS - 1 + len(around))

    for c in (1, 2, 0):
        def out(other_y, other_z, c=c):
            other = other_y * GZ + other_z
            remote(
                send.at[c, pl.ds(pl.multiple_of(other * LZ, LZ), LZ)],
                recv.at[c, gy, mine_z],
                (ssem.at[c], rsem.at[c]),
                {"gy": other_y, "gz": other_z},
            )

        each_peer(gy, gz, out)
        recv[c, gy, mine_z, :] = send[c, mine, :]

    @pl.when(grp == 0)
    def _():
        remote(field_edge_out, field_edge_in, (load_s.at[8], load_s.at[9]), {"grp": 1})

    wave_z, curl_z = waves((N, N), 0)
    wave_y, curl_y = waves((N, N), 1)
    curl_x = me.astype(jnp.float32) * (2.0 * math.pi / N)
    squared = curl_x * curl_x + wave_y * wave_y + wave_z * wave_z
    positive = squared > 0
    scale[0] = jnp.where(positive, 1.0 / jnp.where(positive, squared, 1.0), 0.0)

    @pl.when(me == 0)
    def _():
        base = scale[0]
        top = 1.0 / (squared + math.pi * math.pi)
        scale[0] = 0.5 * (base + top)
        scale[1] = 0.5 * (base - top)

    wait_bytes(y_in, load_s.at[4])
    wait_bytes(z_all, load_s.at[5])
    wait_bytes(x_out, load_s.at[6])
    wait_bytes(x_edge, load_s.at[7])
    curl = (curl_x, curl_y, curl_z)
    table_y = (y_in[0], y_in[1])
    cosine = (z_all[0, 0], z_all[1, 0])
    sine = (z_all[0, 1], z_all[1, 1])

    def transform(plane):
        lines = split(dot3(split(plane), table_y))
        by_cos = dot3(cosine, lines)
        by_sin = dot3(sine, lines)
        real = by_cos[:, :N] + by_sin[:, N:]
        imag = by_cos[:, N:] - by_sin[:, :N]
        return real, imag

    def forward(c):
        wait_bytes(recv2.at[c, pl.ds(0, (PEERS - 1) * LZ)], rsem.at[c])
        plane = jnp.concatenate([recv[c, j] for j in range(GY)], 1)
        real, imag = transform(plane)
        stream[c, 0] = real * scale[0]
        stream[c, 1] = imag * scale[0]

        @pl.when(me == 0)
        def _():
            column = lax.broadcasted_iota(jnp.int32, (N, 2 * N), 1)
            plane = jnp.concatenate([recv[c, j] for j in range(GY)], 1)
            real, imag = transform(jnp.where(column % 128 < LY, plane, -plane))
            stream[c, 0] += real * scale[1]
            stream[c, 1] += imag * scale[1]

    def backward(d):
        a, b = (d + 1) % 3, (d + 2) % 3
        real = curl[b] * stream[a, 1] - curl[a] * stream[b, 1]
        imag = curl[a] * stream[b, 0] - curl[b] * stream[a, 0]
        lines = split(jnp.concatenate([real, imag], 1))
        by_cos = dot3(cosine, lines)
        by_sin = dot3(sine, lines)
        real = by_cos[:, :N] - by_sin[:, N:]
        imag = by_cos[:, N:] + by_sin[:, :N]
        lines = split(jnp.concatenate([real, imag], 1) * (1.0 / (N * N)))
        plane = dot3(lines, table_y, ((1,), (1,)))
        for j in range(GY):
            send2[d, j] = plane[:, 128 * j : 128 * j + 128]

    def send_back(d):
        def out(other_y, other_z):
            remote(
                send2.at[d, other_y, pl.ds(pl.multiple_of(other_z * LZ, LZ), LZ)],
                recv2.at[d, mine],
                (ssem2.at[d], rsem2.at[d]),
                {"gy": other_y, "gz": other_z},
            )

        each_peer(gy, gz, out)
        recv2[d, mine, :] = send2[d, gy, mine_z, :]

    forward(1)
    forward(2)
    backward(0)
    send_back(0)
    forward(0)
    backward(1)
    send_back(1)
    backward(2)

    row = lax.broadcasted_iota(jnp.int32, (LY, N), 0)
    column = lax.broadcasted_iota(jnp.int32, (LY, N), 1)
    tile = lax.broadcasted_iota(jnp.int32, (LY, 128), 1)
    short_row = lax.broadcasted_iota(jnp.int32, (8, N), 0)
    no_wrap_low = jnp.where(is_wake, 0, -N)
    no_wrap_high = jnp.where(is_wake, N, 2 * N)
    first_column = jnp.where(is_wake, 0, -1)
    small_lane = lax.broadcasted_iota(jnp.int32, (LZ, 128), 1)
    small_row = lax.broadcasted_iota(jnp.int32, (LZ, 128), 0)
    last_column = jnp.where(is_wake, N - 1, N)

    def velocity_of(d):
        wait_bytes(recv.at[0, :, pl.ds(0, (PEERS - 1) * LZ // GY)], rsem2.at[d])
        drift = wind[0, d]

        for b in range(2):
            parts = []
            for z in range(4 * b, 4 * b + 4):
                turned = recv2[d, pl.ds(z, HALF, stride=LZ), :].T
                parts.append(jnp.concatenate([turned[:LY], turned[LY:]], 1))
            lines = split(jnp.concatenate(parts, 0))
            out = dot3(lines, (x_out[0], x_out[1])) + drift
            for z in range(4 * b, 4 * b + 4):
                plane = out[LY * (z - 4 * b) : LY * (z - 4 * b) + LY]
                speed[d, z + 1] = plane
                row_out[0, d * LZ + z : d * LZ + z + 1, :] = plane[LY - 1 :]
                row_out[1, d * LZ + z : d * LZ + z + 1, :] = plane[:1]
                if d == 2 and z in (0, 1, LZ - 2, LZ - 1):
                    side, start = (1, 4 * z) if z < 2 else (0, 4 * (z - LZ + 2))
                    near_out[side, start : start + 2, :] = plane[:2]
                    near_out[side, start + 2 : start + 4, :] = plane[LY - 2 :]
            if b == 0:
                remote(
                    speed.at[d, 1],
                    speed.at[d, LZ + 1],
                    (plane_s.at[d], plane_r.at[d]),
                    {"gz": last_z},
                )
        rows = pl.ds(d * LZ, LZ)
        remote(speed.at[d, LZ], speed.at[d, 0], (plane_s.at[d], plane_r.at[d]), {"gz": next_z})
        remote(row_out.at[0, rows], row_in.at[0, rows], (row_s.at[d], row_r.at[d]), {"gy": next_y})
        remote(row_out.at[1, rows], row_in.at[1, rows], (row_s.at[d], row_r.at[d]), {"gy": last_y})
        if d == 2:
            for side, other in ((0, next_z), (1, last_z)):
                remote(near_out.at[side], near_in.at[side], (near_s, near_r), {"gz": other})

        @pl.when(grp == 0)
        def _():
            def add(i, totals):
                for k in range(8):
                    line = 8 * i + k
                    lines = recv2[d, pl.ds(pl.multiple_of(line * LZ, LZ), LZ), :]
                    totals = [t + lines * x_edge[q, pl.ds(line, 1), :] for q, t in enumerate(totals)]
                return tuple(totals)

            zero = jnp.zeros((LZ, 128), jnp.float32)
            totals = lax.fori_loop(0, HALF // 8, add, (zero,) * 4)
            for q in range(4):
                edge_out[d, q] = totals[q] + pltpu.roll(totals[q], LY, 1) + drift
            sems = (edge_s.at[d], edge_r.at[d])
            remote(edge_out.at[d], edge_in.at[d, 0], sems, {"grp": 1})
            for slot in range(1, 5):
                remote(
                    edge_out.at[d, pl.ds(1, 2)],
                    edge_in.at[d, slot, pl.ds(1, 2)],
                    sems,
                    {"grp": 1, **around[slot]},
                )

    def weights(target, d):
        def at(z, carry):
            shift = TIME_STEP * speed[d, z + 1]
            for offset in range(-2, 3):
                value = kernel_weight(offset - shift)
                if d == 0 and offset > 0:
                    value = jnp.where(column >= no_wrap_high - offset, 0.0, value)
                if d == 0 and offset < 0:
                    value = jnp.where(column < no_wrap_low - offset, 0.0, value)
                target[offset + 2, z] = value
            return carry

        lax.fori_loop(0, LZ, at, 0)

    def stretch(d):
        wait_bytes(speed.at[d, pl.ds(0, 2)], plane_r.at[d])
        wait_bytes(row_in.at[0, pl.ds(0, 2 * LZ)], row_r.at[d])

        def at(z, carry):
            here = speed[d, z + 1]
            grad_z = speed[d, z + 2] - speed[d, z]
            low = row_in[0, pl.ds(d * LZ + z, 1), :]
            high = row_in[1, pl.ds(d * LZ + z, 1), :]
            up = jnp.where(row == LY - 1, high, moved_by(here, -1, 0))
            down = jnp.where(row == 0, low, moved_by(here, 1, 0))
            left = moved_by(here, 1, 1)
            left = jnp.concatenate(
                [jnp.where(tile == first_column, 0.0, left[:, :128]), left[:, 128:]], 1
            )
            right = jnp.where(column == last_column, here, moved_by(here, -1, 1))
            strength = field[0, d, z] + (0.5 * TIME_STEP) * (
                field[0, 0, z] * (right - left)
                + field[0, 1, z] * (up - down)
                + field[0, 2, z] * grad_z
            )
            one = moved_by(strength * weight_x[3, z], 1, 1)
            two = moved_by(strength * weight_x[4, z], 2, 1)
            total = strength * weight_x[2, z] + one + two
            total = total + moved_by(strength * weight_x[1, z], -1, 1)
            moved[d, z] = total + moved_by(strength * weight_x[0, z], -2, 1)
            return carry

        lax.fori_loop(0, LZ, at, 0)

    def lateral_send(d):
        @pl.when(is_wake)
        def _():
            wait_bytes(edge_in.at[d, pl.ds(0, 3)], edge_r.at[d])
            if d == 0:
                wait_bytes(field_edge_in, load_s.at[9])

            def particle(q, grad_x):
                here = edge_in[d, 0, q]
                low_y, high_y = edge_in[d, 1, q], edge_in[d, 2, q]
                low_z, high_z = edge_in[d, 3, q], edge_in[d, 4, q]
                up = jnp.where(small_lane == LY - 1, moved_by(high_y, -1, 1), moved_by(here, -1, 1))
                down = jnp.where(small_lane == 0, moved_by(low_y, 1, 1), moved_by(here, 1, 1))
                above = jnp.where(small_row == LZ - 1, moved_by(high_z, -1, 0), moved_by(here, -1, 0))
                below = jnp.where(small_row == 0, moved_by(low_z, 1, 0), moved_by(here, 1, 0))
                return field_edge_in[d, q - 1] + (0.5 * TIME_STEP) * (
                    field_edge_in[0, q - 1] * grad_x
                    + field_edge_in[1, q - 1] * (up - down)
                    + field_edge_in[2, q - 1] * (above - below)
                )

            strength_one = particle(2, edge_in[d, 0, 3] - edge_in[d, 0, 1])
            strength_two = particle(1, edge_in[d, 0, 2] - edge_in[d, 0, 0])
            shift_one = TIME_STEP * edge_in[0, 0, 2]
            shift_two = TIME_STEP * edge_in[0, 0, 1]
            first = strength_one * kernel_weight(1 - shift_one) + strength_two * kernel_weight(
                2 - shift_two
            )
            second = strength_one * kernel_weight(2 - shift_one)
            empty = jnp.zeros((128 - 3 * LZ, 128), jnp.float32)
            turned = jnp.concatenate([edge_in[d, 0, 2], first, second, empty], 0).T[:LY]

            def add(z, carry):
                inflow = jnp.where(tile == 0, pltpu.roll(turned, lax.rem(128 - z, 128), 1), 0.0)
                missing = (-0.5 * TIME_STEP) * field[0, 0, z, :, :128] * inflow
                total = missing * weight_x[2, z, :, :128]
                total = total + pltpu.roll(missing * weight_x[3, z, :, :128], 1, 1)
                total = total + pltpu.roll(missing * weight_x[4, z, :, :128], 2, 1)
                total = total + jnp.where(tile == 0, pltpu.roll(turned, 120 - z, 1), 0.0)
                total = total + jnp.where(tile == 1, pltpu.roll(turned, 113 - z, 1), 0.0)
                moved[d, z, :, :128] += total
                return carry

            lax.fori_loop(0, LZ, add, 0)

        def at(z, carry):
            here = moved[d, z]
            one = moved_by(here * weight_y[3, z], 1, 0)
            two = moved_by(here * weight_y[4, z], 2, 0)
            back_one = moved_by(here * weight_y[1, z], -1, 0)
            back_two = moved_by(here * weight_y[0, z], -2, 0)
            total = here * weight_y[2, z]
            total = total + jnp.where(row < 1, 0.0, one) + jnp.where(row < 2, 0.0, two)
            total = total + jnp.where(row >= LY - 1, 0.0, back_one)
            moved[d, z] = total + jnp.where(row >= LY - 2, 0.0, back_two)
            at_z = pl.ds(d * LZ + z, 1)
            lateral_out[0, 0, at_z, :] = one[0:1] + two[0:1]
            lateral_out[0, 1, at_z, :] = two[1:2]
            lateral_out[1, 0, at_z, :] = back_two[LY - 2 : LY - 1]
            lateral_out[1, 1, at_z, :] = back_one[LY - 1 :] + back_two[LY - 1 :]
            return carry

        lax.fori_loop(0, LZ, at, 0)
        rows = pl.ds(d * LZ, LZ)
        for side, other in ((0, next_y), (1, last_y)):
            for step in range(2):
                remote(
                    lateral_out.at[side, step, rows],
                    lateral_in.at[side, step, rows],
                    (lateral_s.at[d], lateral_r.at[d]),
                    {"gy": other},
                )
        if d == 2:
            for side, other in ((0, next_y), (1, last_y)):
                for level, far in ((0, next_z), (1, last_z)):
                    remote(
                        lateral_out.at[side, :, rows],
                        corner_in.at[side, level],
                        (corner_s, corner_r),
                        {"gy": other, "gz": far},
                    )

    def lateral_rows(d, z):
        at_z = pl.ds(d * LZ + z, 1)
        first, second = lateral_in[0, 0, at_z, :], lateral_in[0, 1, at_z, :]
        third, fourth = lateral_in[1, 0, at_z, :], lateral_in[1, 1, at_z, :]
        low = jnp.where(short_row == 0, first, jnp.where(short_row == 1, second, 0.0))
        high = jnp.where(short_row == 6, third, jnp.where(short_row == 7, fourth, 0.0))
        return low, high

    def lateral_add(d):
        wait_bytes(row_in.at[:, pl.ds(0, 2 * LZ)], lateral_r.at[d])

        def add(z, carry):
            low, high = lateral_rows(d, z)
            moved[d, z, :8] += low
            moved[d, z, LY - 8 :] += high
            return carry

        lax.fori_loop(0, LZ, add, 0)

    def layers_send(d):
        end = LZ - 1
        layer_out[0, d, 0] = moved[d, end] * weight_z[3, end] + moved[d, end - 1] * weight_z[4, end - 1]
        layer_out[0, d, 1] = moved[d, end] * weight_z[4, end]
        layer_out[1, d, 0] = moved[d, 0] * weight_z[0, 0]
        layer_out[1, d, 1] = moved[d, 0] * weight_z[1, 0] + moved[d, 1] * weight_z[0, 1]
        for side, other in ((0, next_z), (1, last_z)):
            remote(
                layer_out.at[side, d],
                layer_in.at[side, d],
                (layer_s.at[d], layer_r.at[d]),
                {"gz": other},
            )
    def layers_within(d):
        for z in range(LZ):
            total = moved[d, z] * weight_z[2, z]
            for offset in (-2, -1, 1, 2):
                if 0 <= z - offset < LZ:
                    total = total + moved[d, z - offset] * weight_z[offset + 2, z - offset]
            result[d, z] = total

    def late_rows(d):
        wait_bytes(row_in.at[:, pl.ds(0, 2 * LZ)], lateral_r.at[d])
        for z in range(LZ):
            for start, part in zip((0, LY - 8), lateral_rows(d, z)):
                rows = slice(start, start + 8)
                for offset in range(-2, 3):
                    if 0 <= z + offset < LZ:
                        result[d, z + offset, rows] += part * weight_z[offset + 2, z, rows]
        wait_bytes(near_in, near_r)
        wait_bytes(corner_in, corner_r)
        for level in range(2):
            for plane in range(2):
                z = plane if level else LZ - 2 + plane
                for side in range(2):
                    for step in range(2):
                        at_row = 4 * plane + 2 * side + step
                        corner[level, at_row : at_row + 1, :] = corner_in[side, level, step, z : z + 1]
        shift = TIME_STEP * near_in[0]
        one = corner[0] * kernel_weight(1 - shift)
        two = corner[0] * kernel_weight(2 - shift)
        parts = [(0, one[4:] + two[:4]), (1, two[4:])]
        shift = TIME_STEP * near_in[1]
        one = corner[1] * kernel_weight(-1 - shift)
        two = corner[1] * kernel_weight(-2 - shift)
        parts += [(LZ - 1, one[:4] + two[4:]), (LZ - 2, two[:4])]
        for z, part in parts:
            result[d, z, :2] += part[:2]
            result[d, z, LY - 2 :] += part[2:]

    def finish(d):
        wait_bytes(layer_in.at[:, d], layer_r.at[d])
        for side, start in ((0, 0), (1, LZ - 2)):
            for step in range(2):
                result[d, start + step] += layer_in[side, d, step]

    velocity_of(0)
    send_back(2)
    weights(weight_x, 0)
    stretch(0)
    velocity_of(1)
    weights(weight_y, 1)
    lateral_send(0)
    stretch(1)
    velocity_of(2)
    weights(weight_z, 2)
    lateral_add(0)
    layers_send(0)
    lateral_send(1)
    stretch(2)
    lateral_add(1)
    layers_send(1)
    lateral_send(2)
    layers_send(2)
    layers_within(0)
    layers_within(1)
    layers_within(2)
    finish(0)
    finish(1)
    late_rows(2)
    finish(2)

    wait_bytes(near_out, near_s)
    wait_bytes(corner_in, corner_s)
    for c in range(3):
        wait_bytes(send.at[c, pl.ds(0, (PEERS - 1) * LZ)], ssem.at[c])
        wait_bytes(send.at[c, pl.ds(0, (PEERS - 1) * LZ)], ssem2.at[c])
        wait_bytes(speed.at[c, pl.ds(0, 2)], plane_s.at[c])
        wait_bytes(row_out.at[0, pl.ds(0, 2 * LZ)], row_s.at[c])
        wait_bytes(row_out.at[:, pl.ds(0, 2 * LZ)], lateral_s.at[c])
        wait_bytes(layer_out.at[:, c], layer_s.at[c])

        @pl.when(grp == 0)
        def _():
            wait_bytes(edge_in.at[c, pl.ds(0, 3)], edge_s.at[c])
            if c == 0:
                wait_bytes(field_edge_out, load_s.at[8])


def output_kernel(result, speed, result_out, velocity_out, sems):
    copies = []
    for d in range(3):
        copies += [
            pltpu.make_async_copy(speed.at[d, pl.ds(1, LZ)], velocity_out.at[0, d], sems.at[d]),
            pltpu.make_async_copy(result.at[d], result_out.at[0, d], sems.at[3 + d]),
        ]
    for copy in copies:
        copy.start()
    for copy in copies:
        copy.wait()


def body(vorticity, wind):
    tables = [jnp.asarray(t) for t in make_tables()]
    anywhere = pl.BlockSpec(memory_space=pl.ANY)
    near = pl.BlockSpec(memory_space=pltpu.VMEM)
    shape = jax.ShapeDtypeStruct(vorticity.shape, jnp.float32)
    block = (3, LZ, LY, N)
    buffers = [
        (3, PEERS * LZ, 128),
        (3, GY, N, 128),
        (3, 2, N, N),
        (3, GY, N, 128),
        (3, PEERS * LZ, 128),
        (2, N, N),
        (5, LZ, LY, N),
        (5, LZ, LY, N),
        (5, LZ, LY, N),
        block,
        (2, 3 * LZ, N),
        (2, 3 * LZ, N),
        (3, 4, LZ, 128),
        (3, 5, 4, LZ, 128),
        (3, 2, LZ, 128),
        (3, 2, LZ, 128),
        (2, 2, 3 * LZ, N),
        (2, 2, 3 * LZ, N),
        (2, 3, 2, LY, N),
        (2, 3, 2, LY, N),
        (2, 8, N),
        (2, 8, N),
        (2, 2, 2, LZ, N),
        (2, 8, N),
    ]
    result, speed = pl.pallas_call(
        step_kernel,
        out_shape=(pltpu.VMEM(block, jnp.float32), pltpu.VMEM((3, LZ + 2, LY, N), jnp.float32)),
        in_specs=[anywhere, pl.BlockSpec(memory_space=pltpu.SMEM)] + [anywhere] * 5,
        out_specs=(pl.BlockSpec(memory_space=pltpu.VMEM), pl.BlockSpec(memory_space=pltpu.VMEM)),
        scratch_shapes=[pltpu.VMEM(vorticity.shape, jnp.float32)]
        + [pltpu.VMEM(t.shape, t.dtype) for t in tables]
        + [pltpu.VMEM(b, jnp.float32) for b in buffers]
        + [pltpu.SemaphoreType.DMA((3,))] * 14
        + [pltpu.SemaphoreType.DMA((10,))]
        + [pltpu.SemaphoreType.DMA] * 4,
        compiler_params=pltpu.CompilerParams(collective_id=0, has_side_effects=True),
    )(vorticity, wind, *tables)
    return pl.pallas_call(
        output_kernel,
        out_shape=(shape, shape),
        in_specs=[near, near],
        out_specs=(anywhere, anywhere),
        scratch_shapes=[pltpu.SemaphoreType.DMA((6,))],
    )(
        pltpu.with_memory_space_constraint(result, pltpu.VMEM),
        pltpu.with_memory_space_constraint(speed, pltpu.VMEM),
    )


def solution(mesh):
    return jax.shard_map(
        body,
        mesh=mesh,
        in_specs=(P("grp", None, "gz", "gy", None), P("grp", None)),
        out_specs=(P("grp", None, "gz", "gy", None), P("grp", None, "gz", "gy", None)),
        check_vma=False,
    )
```
